256 devices in a mesh: grp: 4 (over x, y), tp: 32 (over z), tower: 2 (over core).
Axes of the slice: x: 2, y: 2, z: 32, core: 2. Of those that a mesh axis runs over, the one named last changes fastest.
The devices are a block of a 4x8x32 slice.
Arguments:
- hidden: bfloat16 [2, 4096, 3072], P('tower', ('grp', 'tp')), parts along dimension 1, may hold values from -6 to 6
- modulation: float32 [2, 3, 3072], P('tower'), may hold values from -3 to 7, as said below
- qk_gains: float32 [2, 3, 4096], P('tower', None, 'tp'), may hold values from 0.75 to 13
- counts: int32 [2, 4], P(None, 'grp'), parts along dimension 1, may hold values from 256 to 1024
- offsets: int32 [2, 4], P(None, 'grp'), parts along dimension 1, may hold values from 0 to 8191
- in_weights: bfloat16 [2, 3072, 4, 4096], P('tower', None, None, 'tp'), may hold values from -0.109375 to 0.109375
- out_weights: bfloat16 [2, 2, 4096, 3072], P('tower', None, 'tp'), may hold values from -0.5 to 0.5
Outputs:
- updated: bfloat16 [2, 4096, 3072], P('tower', ('grp', 'tp')), parts along dimension 1
The draws below stay inside these ranges and needn't reach their ends.
There are 4 independent parts, one for each index of `grp`. The reference program is written for one: setup_inputs(seed, part) draws one part's arguments, and reference() takes and returns one part's arrays. A program takes and returns all parts, laid end to end along the dimension named above; an argument that names none is the same for every part. Nothing has to cross between parts.
Inputs may be any that keep to these rules, and one draw needn't show every extreme that they name: `modulation`: rows are shift, scale and gate.
All inputs are finite; a program needn't handle non-finite values.
Results may differ from the reference program's by a relative error of at most 0.025.
The reference program's roundings to bfloat16 on the way (of `normed`, `projected`, `self_out` and `cross_out`) count: a program that leaves them out, or rounds other values in their place, can miss the bound.
Values may be sent and summed in bfloat16 or wider, within the bound.
A program may use at most 64 MiB of HBM per device.

```python
import math
import jax
import jax.numpy as jnp
from jax import lax

D = 3072
HD = 128
TOK = 1024
HEADS = 32
HW = 4096
N_TP = 32


def draw_modulation(key, part):
    first_key, second_key, third_key = jax.random.split(key, 3)
    shift = jnp.clip(0.5 * jax.random.normal(first_key, (2, D), jnp.float32), -3.0, 3.0)
    scale = jnp.clip(0.3 * jax.random.normal(second_key, (2, D), jnp.float32), -0.9, 3.0)
    gate = jax.random.uniform(third_key, (2, D), jnp.float32, 0.5, 1.5)
    return jnp.stack([shift, scale, gate], 1).astype(jnp.float32)


def draw_qk_gains(key, part):
    order_key, placing_key, rough_key = jax.random.split(jax.random.fold_in(key, 17), 3)
    ranking = jax.random.permutation(order_key, HEADS).astype(jnp.float32)
    placing = (ranking + jax.random.uniform(placing_key, (HEADS,), jnp.float32)) / HEADS
    top_log = math.log(2.0)
    head_scale = jnp.exp(top_log * placing)
    roughness = jnp.exp(jax.random.uniform(rough_key, (2, 3, HEADS, HD), jnp.float32, -0.25, 0.25))
    return (head_scale[None, None, :, None] * roughness).reshape(2, 3, HW).astype(jnp.float32)


def level_of(own_key, extent, cuts, low, high):
    loudness, own = 1.0, jax.random.fold_in(own_key, 6)
    for dim, parts in cuts:
        draws = jnp.exp(jax.random.uniform(jax.random.fold_in(own, dim), (parts,), jnp.float32, low / len(cuts), high / len(cuts)))
        loudness = loudness * jnp.repeat(draws, extent[dim] // parts).reshape([-1 if axis == dim else 1 for axis in range(len(extent))])
    return loudness


def scatter_about(stream_key, dims, scale, most, shards=(), kind=jnp.bfloat16):
    entries = jax.random.normal(stream_key, dims, jnp.float32) * scale
    if len(shards) > 0:
        entries = level_of(stream_key, dims, shards, -0.22, 0.18) * entries
    return jnp.clip(entries, min=-most, max=most).astype(kind)


def setup_inputs(seed: int = 0, part: int = 0) -> dict:
    splits = jax.random.split(jax.random.key(seed), 8)
    own_keys = jax.random.split(jax.random.fold_in(splits[7], part), 8)
    hidden = scatter_about(own_keys[0], (2, TOK, D), 1.0, 6.0, ((0, 2), (1, 32)))
    modulation = draw_modulation(jax.random.fold_in(splits[7], 71), part)
    qk_gains = draw_qk_gains(jax.random.fold_in(splits[7], 71), part)
    counts = jax.random.randint(own_keys[3], (2, 1), TOK // 4, TOK + 1).astype(jnp.int32)
    offsets = jax.random.randint(own_keys[4], (2, 1), 0, 8192).astype(jnp.int32)
    in_weights = scatter_about(splits[5], (2, D, 4, HW), D ** -0.5, 0.109375, ((0, 2), (3, 32)))
    out_weights = scatter_about(splits[6], (2, 2, HW, D), HD ** -0.5, 0.5, ((0, 2), (2, 32)))
    return {"hidden": hidden, "modulation": modulation, "qk_gains": qk_gains, "counts": counts, "offsets": offsets, "in_weights": in_weights, "out_weights": out_weights}


epsilon = 1e-06
rope_base = 10000.0
masked_score = -1e+30

def layer_norm(states):
    centre = states - lax.optimization_barrier(jnp.mean(states, -1, keepdims=True))
    spread = lax.optimization_barrier(jnp.mean(centre * centre, -1, keepdims=True))
    return centre * lax.rsqrt(spread + epsilon)

def rotate(columns, positions):
    head_width = columns.shape[-1]
    pair_index = jnp.arange(head_width // 2, dtype=jnp.int32)
    frequency = jnp.exp(pair_index.astype(jnp.float32) * (-2.0 * math.log(rope_base) / head_width))
    angles = positions.reshape((positions.shape[0],) + (1,) * (columns.ndim - 1)) * frequency
    cosine = jnp.cos(angles)
    sine_table = jnp.sin(angles)
    even_part = columns[..., 0::2]
    odd_part = columns[..., 1::2]
    turned = jnp.stack([even_part * cosine - odd_part * sine_table, even_part * sine_table + odd_part * cosine], -1)
    return turned.reshape(columns.shape)

def finish(projected, head_gains, positions):
    query_like = jnp.stack([projected[:, 0], projected[:, 1], projected[:, 3]], 1)
    squares = lax.optimization_barrier(jnp.mean(query_like * query_like, -1, keepdims=True))
    query_like = query_like * lax.rsqrt(squares + epsilon) * head_gains[None]
    turned = rotate(query_like, positions)
    return jnp.stack([turned[:, 0], turned[:, 1], projected[:, 2], turned[:, 2]], 1)

def attend(queries, key_rows, value_rows, key_count):
    scores = jnp.dot(queries, key_rows.T, preferred_element_type=jnp.float32) * (1.0 / math.sqrt(queries.shape[-1]))
    usable = jnp.arange(key_rows.shape[0], dtype=jnp.int32) < key_count
    scores = jnp.where(usable[None, :], scores, masked_score)
    row_max = lax.optimization_barrier(jnp.max(scores, -1, keepdims=True))
    raised = jnp.exp(scores - row_max)
    attention = (raised / lax.optimization_barrier(jnp.sum(raised, -1, keepdims=True))).astype(jnp.bfloat16)
    return jnp.dot(attention, value_rows, preferred_element_type=jnp.float32).astype(jnp.bfloat16)

def prepare(tower_index, hidden, modulation, qk_gains, offsets, in_weights):
    states = hidden[tower_index].astype(jnp.float32)
    modulate = modulation[tower_index]
    normed = (layer_norm(states) * (1.0 + modulate[1]) + modulate[0]).astype(jnp.bfloat16)
    projected = jnp.dot(normed, in_weights[tower_index].reshape(D, 4 * HW), preferred_element_type=jnp.float32)
    positions = (offsets[tower_index, 0] + jnp.arange(TOK, dtype=jnp.int32)).astype(jnp.float32)
    head_gains = qk_gains[tower_index].reshape(3, HEADS, HD)
    finished = finish(projected.reshape(TOK, 4, HEADS, HD), head_gains, positions)
    return (states, modulate, finished.astype(jnp.bfloat16))

def heads_attend(queries, key_rows, value_rows, key_count):
    stacked = (jnp.swapaxes(queries, 0, 1), jnp.swapaxes(key_rows, 0, 1), jnp.swapaxes(value_rows, 0, 1))
    result = lax.map(lambda triple: attend(triple[0], triple[1], triple[2], key_count), stacked)
    return jnp.swapaxes(result, 0, 1).reshape(queries.shape[0], HW)

def branch_sum(self_out, cross_out, weights):
    block_width = HW // N_TP

    def accumulate(total_sum, block_index):
        row_start = block_index * block_width
        self_part = lax.dynamic_slice_in_dim(self_out, row_start, block_width, 1)
        cross_part = lax.dynamic_slice_in_dim(cross_out, row_start, block_width, 1)
        self_weight = lax.dynamic_slice_in_dim(weights[0], row_start, block_width, 0)
        cross_weight = lax.dynamic_slice_in_dim(weights[1], row_start, block_width, 0)
        partial_term = jnp.dot(self_part, self_weight, preferred_element_type=jnp.float32) + jnp.dot(cross_part, cross_weight, preferred_element_type=jnp.float32)
        rounded = lax.optimization_barrier(partial_term.astype(jnp.bfloat16))
        return (total_sum + rounded.astype(jnp.float32), None)
    total_sum, unused = lax.scan(accumulate, jnp.zeros((TOK, D), jnp.float32), jnp.arange(N_TP, dtype=jnp.int32))
    return total_sum

def reference(hidden, modulation, qk_gains, counts, offsets, in_weights, out_weights):
    prepared = [prepare(tower_index, hidden, modulation, qk_gains, offsets, in_weights) for tower_index in range(2)]
    outputs = []
    for tower_index in range(2):
        states, modulate, projected = prepared[tower_index]
        opposite = prepared[1 - tower_index][2]
        self_out = heads_attend(projected[:, 0], projected[:, 1], projected[:, 2], counts[tower_index, 0])
        cross_out = heads_attend(projected[:, 3], opposite[:, 1], opposite[:, 2], counts[1 - tower_index, 0])
        branch = branch_sum(self_out, cross_out, out_weights[tower_index])
        outputs.append((states + modulate[2] * branch).astype(jnp.bfloat16))
    return jnp.stack(outputs, 0)
```

```python
import functools
import math

import jax
import jax.numpy as jnp
import numpy as np
from jax import lax
from jax.experimental import pallas as pl
from jax.experimental.pallas import tpu as pltpu
from jax.sharding import PartitionSpec as P

MESH = pl.DeviceIdType.MESH
epsilon = 1e-06
rope_base = 10000.0
masked_score = -1e30
CHUNKS = 4


def kernel(
    n,
    h_ref,
    mod_ref,
    gain_ref,
    freq_ref,
    cnt_ref,
    off_ref,
    win_ref,
    wout_ref,
    out_ref,
    rows_all,
    raw,
    wide,
    w_in,
    w_out,
    acc,
    q_all,
    c_all,
    kv_own,
    kv_far,
    bias,
    both,
    part,
    rs_in,
    rs_out,
    w_sem,
    ag_send,
    ag_recv,
    kv_send,
    kv_recv,
    rs_send,
    rs_recv,
):
    half = n // 2
    me = lax.axis_index("tp")
    tower = lax.axis_index("tower")
    right = lax.rem(me + 1, n)
    left = lax.rem(me + n - 1, n)
    other = 1 - tower
    rows, width = h_ref.shape
    head = gain_ref.shape[-1]
    cols = width // CHUNKS
    tokens = n * rows
    score_scale = math.log2(math.e) / math.sqrt(head)

    win_copy = pltpu.make_async_copy(win_ref, raw, w_sem.at[0])
    wout_copy = pltpu.make_async_copy(wout_ref, w_out, w_sem.at[1])
    win_copy.start()
    wout_copy.start()

    barrier = pltpu.get_barrier_semaphore()
    for where in ({"tp": left}, {"tp": right}, {"tower": other}):
        pl.semaphore_signal(barrier, inc=1, device_id=where, device_id_type=MESH)

    def block(offset):
        return lax.rem(me + offset + 2 * n, n)

    def gather_copy(way, step, i):
        b = block(-step if way == 0 else step)
        return pltpu.make_async_remote_copy(
            src_ref=rows_all.at[b, i],
            dst_ref=rows_all.at[b, i],
            send_sem=ag_send.at[way, step, i],
            recv_sem=ag_recv.at[way, step, i],
            device_id={"tp": right if way == 0 else left},
            device_id_type=MESH,
        )

    def gather_arrival(way, step, i):
        b = block(-step if way == 0 else step)
        return pltpu.make_async_remote_copy(
            src_ref=rows_all.at[b, i],
            dst_ref=rows_all.at[b, i],
            send_sem=ag_send.at[way, step - 1, i],
            recv_sem=ag_recv.at[way, step - 1, i],
            device_id={"tp": right if way == 0 else left},
            device_id_type=MESH,
        )

    def kv_copy(b):
        return pltpu.make_async_remote_copy(
            src_ref=kv_own.at[b],
            dst_ref=kv_far.at[b],
            send_sem=kv_send.at[b],
            recv_sem=kv_recv.at[b],
            device_id={"tower": other},
            device_id_type=MESH,
        )

    def scatter_copy(way, step, i):
        return pltpu.make_async_remote_copy(
            src_ref=rs_out.at[way, step, i],
            dst_ref=rs_in.at[way, step, i],
            send_sem=rs_send.at[way, step, i],
            recv_sem=rs_recv.at[way, step, i],
            device_id={"tp": right if way == 0 else left},
            device_id_type=MESH,
        )

    states = h_ref[...].astype(jnp.float32)
    centre = states - jnp.mean(states, -1, keepdims=True)
    spread = jnp.mean(centre * centre, -1, keepdims=True)
    normed = centre * lax.rsqrt(spread + epsilon) * (1.0 + mod_ref[1:2, :]) + mod_ref[0:1, :]
    normed = normed.astype(jnp.bfloat16)
    for i in range(CHUNKS):
        rows_all[me, i] = normed[:, i * cols : (i + 1) * cols]

    key_index = lax.broadcasted_iota(jnp.int32, (1, tokens), 1)
    bias[0:1, :] = jnp.where(key_index < cnt_ref[tower, 0], 0.0, masked_score)
    bias[1:2, :] = jnp.where(key_index < cnt_ref[other, 0], 0.0, masked_score)

    pl.semaphore_wait(barrier, 3)
    for i in range(CHUNKS):
        gather_copy(0, 0, i).start()
        gather_copy(1, 0, i).start()

    win_copy.wait()
    fold = wide.shape[0] // 4

    def unfold(j, carry):
        wide[...] = raw[pl.ds(pl.multiple_of(j * 4 * fold, 4 * fold), 4 * fold), :].astype(jnp.float32)
        for c in range(4):
            w_in[pl.ds(pl.multiple_of(j * fold, fold), fold), c * head : (c + 1) * head] = wide[
                pl.ds(c, fold, stride=4), :
            ].astype(jnp.bfloat16)
        return carry

    lax.fori_loop(0, width // fold, unfold, 0)
    wout_copy.wait()

    lane = lax.broadcasted_iota(jnp.int32, (1, head), 1)
    is_even = lax.rem(lane, 2) == 0
    offset = off_ref[tower, 0]

    def row_positions(b):
        return offset + b * rows + lax.broadcasted_iota(jnp.int32, (rows, 1), 0)

    def project(i, blocks):
        picked = [rows_all[b, i] for b in blocks]
        lhs = picked[0] if len(picked) == 1 else jnp.concatenate(picked, 0)
        term = jnp.dot(lhs, w_in[i * cols : (i + 1) * cols, :], preferred_element_type=jnp.float32)
        if i == 0:
            acc[: lhs.shape[0], :] = term
        else:
            acc[: lhs.shape[0], :] += term

    def finish(blocks):
        count = len(blocks) * rows
        positions = [row_positions(b) for b in blocks]
        positions = positions[0] if len(blocks) == 1 else jnp.concatenate(positions, 0)
        angles = positions.astype(jnp.float32) * freq_ref[...]
        cosine = jnp.cos(angles)
        sine = jnp.sin(angles)
        sine = jnp.where(is_even, -sine, sine)

        def turned(c, g):
            x = acc[:count, c * head : (c + 1) * head]
            square = jnp.mean(x * x, -1, keepdims=True)
            x = x * lax.rsqrt(square + epsilon) * gain_ref[g : g + 1, :]
            swapped = jnp.where(is_even, pltpu.roll(x, head - 1, 1), pltpu.roll(x, 1, 1))
            return (x * cosine + swapped * sine).astype(jnp.bfloat16)

        queries = turned(0, 0)
        keys = turned(1, 1)
        values = acc[:count, 2 * head : 3 * head].astype(jnp.bfloat16)
        cross = turned(3, 2)
        for j, b in enumerate(blocks):
            span = slice(j * rows, (j + 1) * rows)
            q_all[b] = queries[span]
            kv_own[b, 0] = keys[span]
            kv_own[b, 1] = values[span]
            c_all[b] = cross[span]

    for i in range(CHUNKS):
        project(i, [me])
    finish([me])

    def gather_step(step, carry):
        before, after = block(-step), block(step)
        for i in range(CHUNKS):
            gather_arrival(0, step, i).wait_recv()
            if i < CHUNKS // 2:
                gather_copy(0, step, i).start()
            else:
                pl.when(step < half - 1)(lambda i=i: gather_copy(0, step, i).start())
            gather_arrival(1, step, i).wait_recv()
            if i < CHUNKS // 2:
                pl.when(step < half - 1)(lambda i=i: gather_copy(1, step, i).start())
            else:
                gather_copy(1, step, i).start()
            if i == 1:
                kv_copy(block(1 - step)).start()
                pl.when(step > 1)(lambda: kv_copy(block(step - 1)).start())
            project(i, [before, after])
        finish([before, after])
        return carry

    lax.fori_loop(1, half, gather_step, 0)
    kv_copy(block(1 - half)).start()
    kv_copy(block(half - 1)).start()
    last = block(half)
    for i in range(CHUNKS):
        gather_arrival(0 if i < CHUNKS // 2 else 1, half, i).wait_recv()
        project(i, [last])
    finish([last])

    def attend(queries, pairs, row):
        keys = pairs[:, 0].reshape(tokens, head)
        values = pairs[:, 1].reshape(tokens, head)
        scores = lax.dot_general(
            queries, keys, (((1,), (1,)), ((), ())), preferred_element_type=jnp.float32
        )
        scores = scores * score_scale + bias[row : row + 1, :]
        raised = jnp.exp2(scores - jnp.max(scores, -1, keepdims=True))
        total = jnp.sum(raised, -1, keepdims=True)
        summed = jnp.dot(raised.astype(jnp.bfloat16), values, preferred_element_type=jnp.float32)
        return (summed / total).astype(jnp.bfloat16)

    def attend_self(blocks):
        picked = [q_all[b] for b in blocks]
        lhs = picked[0] if len(picked) == 1 else jnp.concatenate(picked, 0)
        both[: lhs.shape[0], :head] = attend(lhs, kv_own, 0)

    def attend_cross(blocks):
        picked = [c_all[b] for b in blocks]
        lhs = picked[0] if len(picked) == 1 else jnp.concatenate(picked, 0)
        both[: lhs.shape[0], head:] = attend(lhs, kv_far, 1)

    def expand(count, i):
        return jnp.dot(
            both[:count, :], w_out[:, i * cols : (i + 1) * cols], preferred_element_type=jnp.float32
        )

    def partial_piece(slot, blocks, piece):
        if piece == 0:
            attend_self(blocks)
        elif piece == 1:
            attend_cross(blocks)
        else:
            for i in range(2 * (piece - 2), 2 * (piece - 1)):
                term = expand(2 * rows, i)
                part[slot, 0, i] = term[:rows]
                part[slot, 1, i] = term[rows:]

    attend_self([last])
    kv_copy(last).start()
    quiet = jnp.zeros((rows, cols), jnp.bfloat16)
    for i in range(CHUNKS):
        rs_in[1 if i < CHUNKS // 2 else 0, 0, i] = quiet

    def take_far(b, carry):
        kv_copy(b).wait_recv()
        return carry

    lax.fori_loop(0, n, take_far, 0)
    attend_cross([last])
    for i in range(CHUNKS):
        way = 0 if i < CHUNKS // 2 else 1
        rs_out[way, 0, i] = expand(rows, i).astype(jnp.bfloat16)
    for i in range(CHUNKS):
        scatter_copy(0 if i < CHUNKS // 2 else 1, 0, i).start()
    for piece in range(4):
        partial_piece(1, [block(half - 1), block(1 - half)], piece)

    def scatter_step(step, carry):
        slot = lax.rem(step, 2)
        following = [block(half - 1 - step), block(step + 1 - half)]
        for i in range(CHUNKS):
            for way in range(2):
                if (i < CHUNKS // 2) == (way == 0):
                    scatter_copy(way, step - 1, i).wait_recv()
                else:
                    pl.when(step > 1)(lambda way=way, i=i: scatter_copy(way, step - 1, i).wait_recv())
                running = rs_in[way, step - 1, i].astype(jnp.float32) + part[slot, way, i]
                rs_out[way, step, i] = running.astype(jnp.bfloat16)
                scatter_copy(way, step, i).start()
            partial_piece(1 - slot, following, i)
        return carry

    lax.fori_loop(1, half, scatter_step, 0)
    for i in range(CHUNKS):
        scatter_copy(0, half - 1, i).wait_recv()
        scatter_copy(1, half - 1, i).wait_recv()
        span = slice(i * cols, (i + 1) * cols)
        branch = part[half % 2, 0, i] + (
            rs_in[0, half - 1, i].astype(jnp.float32) + rs_in[1, half - 1, i].astype(jnp.float32)
        )
        out_ref[:, span] = (
            h_ref[:, span].astype(jnp.float32) + mod_ref[2:3, span] * branch
        ).astype(jnp.bfloat16)

    def settle(step, carry):
        for i in range(CHUNKS):
            for way in range(2):
                near = (i < CHUNKS // 2) == (way == 0)
                if near:
                    gather_copy(way, step, i).wait_send()
                    scatter_copy(way, step, i).wait_send()
                else:
                    pl.when(step < half - 1)(lambda way=way, i=i: gather_copy(way, step, i).wait_send())
                    pl.when(step > 0)(lambda way=way, i=i: scatter_copy(way, step, i).wait_send())
        return carry

    lax.fori_loop(0, half, settle, 0)

    def settle_far(b, carry):
        kv_copy(b).wait_send()
        return carry

    lax.fori_loop(0, n, settle_far, 0)


def local(n, hidden, modulation, qk_gains, counts, offsets, in_weights, out_weights):
    rows, width = hidden.shape[1:]
    head = in_weights.shape[-1]
    half = n // 2
    tokens = n * rows
    cols = width // CHUNKS
    frequency = np.repeat(
        np.exp(np.arange(head // 2, dtype=np.float64) * (-2.0 * math.log(rope_base) / head)), 2
    ).astype(np.float32)[None]
    vmem = pl.BlockSpec(memory_space=pltpu.VMEM)
    smem = pl.BlockSpec(memory_space=pltpu.SMEM)
    anywhere = pl.BlockSpec(memory_space=pl.ANY)
    updated = pl.pallas_call(
        functools.partial(kernel, n),
        out_shape=jax.ShapeDtypeStruct((rows, width), jnp.bfloat16),
        in_specs=[vmem, vmem, vmem, vmem, smem, smem, anywhere, anywhere],
        out_specs=vmem,
        scratch_shapes=[
            pltpu.VMEM((n, CHUNKS, rows, cols), jnp.bfloat16),
            pltpu.VMEM((width * 4, head), jnp.bfloat16),
            pltpu.VMEM((4 * 128, head), jnp.float32),
            pltpu.VMEM((width, 4 * head), jnp.bfloat16),
            pltpu.VMEM((2 * head, width), jnp.bfloat16),
            pltpu.VMEM((2 * rows, 4 * head), jnp.float32),
            pltpu.VMEM((n, rows, head), jnp.bfloat16),
            pltpu.VMEM((n, rows, head), jnp.bfloat16),
            pltpu.VMEM((n, 2, rows, head), jnp.bfloat16),
            pltpu.VMEM((n, 2, rows, head), jnp.bfloat16),
            pltpu.VMEM((2, tokens), jnp.float32),
            pltpu.VMEM((2 * rows, 2 * head), jnp.bfloat16),
            pltpu.VMEM((2, 2, CHUNKS, rows, cols), jnp.float32),
            pltpu.VMEM((2, half, CHUNKS, rows, cols), jnp.bfloat16),
            pltpu.VMEM((2, half, CHUNKS, rows, cols), jnp.bfloat16),
            pltpu.SemaphoreType.DMA((2,)),
            pltpu.SemaphoreType.DMA((2, half, CHUNKS)),
            pltpu.SemaphoreType.DMA((2, half, CHUNKS)),
            pltpu.SemaphoreType.DMA((n,)),
            pltpu.SemaphoreType.DMA((n,)),
            pltpu.SemaphoreType.DMA((2, half, CHUNKS)),
            pltpu.SemaphoreType.DMA((2, half, CHUNKS)),
        ],
        compiler_params=pltpu.CompilerParams(
            collective_id=0, has_side_effects=True, vmem_limit_bytes=56 * 1024 * 1024
        ),
    )(
        hidden[0],
        modulation[0],
        qk_gains[0].reshape(3, head),
        jnp.asarray(frequency),
        counts,
        offsets,
        in_weights.reshape(4 * width, head),
        out_weights.reshape(2 * head, width),
    )
    return updated[None]


def solution(mesh):
    return jax.shard_map(
        functools.partial(local, mesh.shape["tp"]),
        mesh=mesh,
        in_specs=(
            P("tower", ("grp", "tp"), None),
            P("tower", None, None),
            P("tower", None, "tp"),
            P(None, "grp"),
            P(None, "grp"),
            P("tower", None, None, "tp"),
            P("tower", None, "tp", None),
        ),
        out_specs=P("tower", ("grp", "tp"), None),
        check_vma=False,
    )
```

```python
import functools
import math

import jax
import jax.numpy as jnp
import numpy as np
from jax import lax
from jax.experimental import pallas as pl
from jax.experimental.pallas import tpu as pltpu
from jax.sharding import PartitionSpec as P

MESH = pl.DeviceIdType.MESH
epsilon = 1e-06
rope_base = 10000.0
masked_score = -1e30
CHUNKS = 4


def kernel(
    n,
    h_hbm,
    mod_hbm,
    gain_hbm,
    freq_hbm,
    cnt_hbm,
    off_hbm,
    win_hbm,
    wout_hbm,
    out_ref,
    h_ref,
    mod_ref,
    gain_ref,
    freq_ref,
    cnt_ref,
    off_ref,
    rows_all,
    raw,
    wide,
    w_in,
    w_out,
    acc,
    q_all,
    c_all,
    kv_own,
    kv_far,
    bias,
    trig,
    both,
    part,
    rs_in,
    rs_out,
    w_sem,
    out_sem,
    ag_recv,
    kv_recv,
    rs_recv,
):
    half = n // 2
    me = lax.axis_index("tp")
    tower = lax.axis_index("tower")
    right = lax.rem(me + 1, n)
    left = lax.rem(me + n - 1, n)
    other = 1 - tower
    depth = rs_recv.shape[1]
    rows, width = h_ref.shape
    head = gain_ref.shape[-1]
    cols = width // CHUNKS
    tokens = n * rows
    score_scale = math.log2(math.e) / math.sqrt(head)

    loads = [
        pltpu.make_async_copy(source, target, w_sem.at[j])
        for j, (source, target) in enumerate(
            (
                (h_hbm, h_ref),
                (mod_hbm, mod_ref),
                (win_hbm, raw),
                (cnt_hbm, cnt_ref),
                (off_hbm, off_ref),
                (gain_hbm, gain_ref),
                (freq_hbm, freq_ref),
                (wout_hbm, w_out),
            )
        )
    ]
    h_copy, mod_copy, win_copy, cnt_copy, off_copy, gain_copy, freq_copy, wout_copy = loads
    for load in loads:
        load.start()

    barrier = pltpu.get_barrier_semaphore()
    for where in ({"tp": left}, {"tp": right}, {"tower": other}):
        pl.semaphore_signal(barrier, inc=1, device_id=where, device_id_type=MESH)

    def block(offset):
        return lax.rem(me + offset + 2 * n, n)

    def gather_copy(way, step, i):
        piece = block(-step if way == 0 else step) * CHUNKS + i
        return pltpu.make_async_remote_copy(
            src_ref=rows_all.at[piece],
            dst_ref=rows_all.at[piece],
            send_sem=out_sem.at[0],
            recv_sem=ag_recv.at[way, lax.rem(step, depth), i],
            device_id={"tp": right if way == 0 else left},
            device_id_type=MESH,
        )

    def gather_arrival(way, step, i):
        return gather_copy(way, step - 1, i)

    def kv_copy(b):
        return pltpu.make_async_remote_copy(
            src_ref=kv_own.at[b],
            dst_ref=kv_far.at[b],
            send_sem=out_sem.at[1],
            recv_sem=kv_recv,
            device_id={"tower": other},
            device_id_type=MESH,
        )

    def scatter_copy(way, step, i):
        piece = (way * half + step) * CHUNKS + i
        return pltpu.make_async_remote_copy(
            src_ref=rs_out.at[piece],
            dst_ref=rs_in.at[piece],
            send_sem=out_sem.at[2],
            recv_sem=rs_recv.at[way, lax.rem(step, depth), i],
            device_id={"tp": right if way == 0 else left},
            device_id_type=MESH,
        )

    def all_sent(ref, count, sem):
        return pltpu.make_async_remote_copy(
            src_ref=ref.at[pl.ds(0, count)],
            dst_ref=ref.at[pl.ds(0, count)],
            send_sem=sem,
            recv_sem=kv_recv,
            device_id={"tower": other},
            device_id_type=MESH,
        )

    h_copy.wait()
    mod_copy.wait()
    states = h_ref[...].astype(jnp.float32)
    centre = states - jnp.mean(states, -1, keepdims=True)
    spread = jnp.mean(centre * centre, -1, keepdims=True)
    normed = centre * lax.rsqrt(spread + epsilon) * (1.0 + mod_ref[1]) + mod_ref[0]
    normed = normed.astype(jnp.bfloat16)
    for i in range(CHUNKS):
        rows_all[me * CHUNKS + i] = normed[:, i * cols : (i + 1) * cols]

    pl.semaphore_wait(barrier, 3)
    for i in range(CHUNKS):
        gather_copy(0, 0, i).start()
        gather_copy(1, 0, i).start()

    cnt_copy.wait()
    key_index = lax.broadcasted_iota(jnp.int32, (1, tokens), 1)
    bias[0:1, :] = jnp.where(key_index < cnt_ref[0, tower], 0.0, masked_score)
    bias[1:2, :] = jnp.where(key_index < cnt_ref[0, other], 0.0, masked_score)

    win_copy.wait()
    fold = wide.shape[0] // 4

    def unfold(j, carry):
        wide[...] = raw[pl.ds(pl.multiple_of(j * 4 * fold, 4 * fold), 4 * fold), :].astype(jnp.float32)
        for c in range(4):
            w_in[pl.ds(pl.multiple_of(j * fold, fold), fold), c * head : (c + 1) * head] = wide[
                pl.ds(c, fold, stride=4), :
            ].astype(jnp.bfloat16)
        return carry

    lax.fori_loop(0, width // fold, unfold, 0)
    for load in (off_copy, gain_copy, freq_copy, wout_copy):
        load.wait()

    lane = lax.broadcasted_iota(jnp.int32, (1, head), 1)
    is_even = lax.rem(lane, 2) == 0
    offset = off_ref[0, tower]

    def row_positions(b):
        return offset + b * rows + lax.broadcasted_iota(jnp.int32, (rows, 1), 0)

    def project(i, blocks):
        picked = [rows_all[b * CHUNKS + i] for b in blocks]
        lhs = picked[0] if len(picked) == 1 else jnp.concatenate(picked, 0)
        term = jnp.dot(lhs, w_in[i * cols : (i + 1) * cols, :], preferred_element_type=jnp.float32)
        if i == 0:
            acc[: lhs.shape[0], :] = term
        else:
            acc[: lhs.shape[0], :] += term

    def prepare_turn(blocks):
        for j, b in enumerate(blocks):
            angles = row_positions(b).astype(jnp.float32) * freq_ref[...]
            sine = jnp.sin(angles)
            trig[0, j * rows : (j + 1) * rows] = jnp.cos(angles)
            trig[1, j * rows : (j + 1) * rows] = jnp.where(is_even, -sine, sine)

    def finish(blocks):
        count = len(blocks) * rows
        cosine = trig[0, :count]
        sine = trig[1, :count]

        def turned(c, g):
            x = acc[:count, c * head : (c + 1) * head]
            square = jnp.mean(x * x, -1, keepdims=True)
            x = x * lax.rsqrt(square + epsilon) * gain_ref[g]
            swapped = jnp.where(is_even, pltpu.roll(x, head - 1, 1), pltpu.roll(x, 1, 1))
            return (x * cosine + swapped * sine).astype(jnp.bfloat16)

        keys = turned(1, 1)
        values = acc[:count, 2 * head : 3 * head].astype(jnp.bfloat16)
        for j, b in enumerate(blocks):
            span = slice(j * rows, (j + 1) * rows)
            kv_own[b, 0] = keys[span]
            kv_own[b, 1] = values[span]
        queries = turned(0, 0)
        cross = turned(3, 2)
        for j, b in enumerate(blocks):
            span = slice(j * rows, (j + 1) * rows)
            q_all[b] = queries[span]
            c_all[b] = cross[span]

    for i in range(CHUNKS):
        project(i, [me])
    prepare_turn([me])
    finish([me])

    def gather_step(step, carry):
        before, after = block(-step), block(step)
        prepare_turn([before, after])
        for i in range(CHUNKS):
            gather_arrival(0, step, i).wait_recv()
            if i < CHUNKS // 2:
                gather_copy(0, step, i).start()
            else:
                pl.when(step < half - 1)(lambda i=i: gather_copy(0, step, i).start())
            gather_arrival(1, step, i).wait_recv()
            if i < CHUNKS // 2:
                pl.when(step < half - 1)(lambda i=i: gather_copy(1, step, i).start())
            else:
                gather_copy(1, step, i).start()
            if i == 1:
                kv_copy(block(1 - step)).start()
                pl.when(step > 1)(lambda: kv_copy(block(step - 1)).start())
            project(i, [before, after])
        finish([before, after])
        return carry

    lax.fori_loop(1, half, gather_step, 0)
    kv_copy(block(1 - half)).start()
    kv_copy(block(half - 1)).start()
    last = block(half)
    prepare_turn([last])
    quiet = jnp.zeros((rows, cols), jnp.bfloat16)
    for i in range(CHUNKS):
        rs_in[(half if i < CHUNKS // 2 else 0) * CHUNKS + i] = quiet
    for i in range(CHUNKS):
        gather_arrival(0 if i < CHUNKS // 2 else 1, half, i).wait_recv()
        project(i, [last])
    finish([last])
    kv_copy(last).start()

    def attend(queries, pairs, row):
        keys = pairs[:, 0].reshape(tokens, head)
        values = pairs[:, 1].reshape(tokens, head)
        scores = lax.dot_general(
            queries, keys, (((1,), (1,)), ((), ())), preferred_element_type=jnp.float32
        )
        scores = scores * score_scale + bias[row : row + 1, :]
        raised = jnp.exp2(scores - jnp.max(scores, -1, keepdims=True))
        total = jnp.sum(raised, -1, keepdims=True)
        summed = jnp.dot(raised.astype(jnp.bfloat16), values, preferred_element_type=jnp.float32)
        return (summed / total).astype(jnp.bfloat16)

    def attend_self(blocks):
        picked = [q_all[b] for b in blocks]
        lhs = picked[0] if len(picked) == 1 else jnp.concatenate(picked, 0)
        both[: lhs.shape[0], :head] = attend(lhs, kv_own, 0)

    def attend_cross(blocks):
        picked = [c_all[b] for b in blocks]
        lhs = picked[0] if len(picked) == 1 else jnp.concatenate(picked, 0)
        both[: lhs.shape[0], head:] = attend(lhs, kv_far, 1)

    def expand(count, i):
        return jnp.dot(
            both[:count, :], w_out[:, i * cols : (i + 1) * cols], preferred_element_type=jnp.float32
        )

    def partial_piece(slot, blocks, piece):
        if piece == 0:
            attend_self(blocks)
        elif piece == 1:
            attend_cross(blocks)
        else:
            for i in range(2 * (piece - 2), 2 * (piece - 1)):
                term = expand(2 * rows, i)
                part[slot, 0, i] = term[:rows]
                part[slot, 1, i] = term[rows:]

    attend_self([last])
    pltpu.make_async_copy(kv_far, kv_far, kv_recv).wait()
    attend_cross([last])
    for i in (0, 2, 1, 3):
        way = 0 if i < CHUNKS // 2 else 1
        rs_out[way * half * CHUNKS + i] = expand(rows, i).astype(jnp.bfloat16)
        scatter_copy(way, 0, i).start()
    for piece in range(4):
        partial_piece(1, [block(half - 1), block(1 - half)], piece)

    def scatter_step(step, carry):
        slot = lax.rem(step, 2)
        following = [block(half - 1 - step), block(step + 1 - half)]
        for i in range(CHUNKS):
            for way in range(2):
                if (i < CHUNKS // 2) == (way == 0):
                    scatter_copy(way, step - 1, i).wait_recv()
                else:
                    pl.when(step > 1)(lambda way=way, i=i: scatter_copy(way, step - 1, i).wait_recv())
                running = rs_in[(way * half + step - 1) * CHUNKS + i].astype(jnp.float32) + part[slot, way, i]
                rs_out[(way * half + step) * CHUNKS + i] = running.astype(jnp.bfloat16)
                scatter_copy(way, step, i).start()
            partial_piece(1 - slot, following, i)
        return carry

    lax.fori_loop(1, half, scatter_step, 0)
    for i in range(CHUNKS):
        scatter_copy(0, half - 1, i).wait_recv()
        scatter_copy(1, half - 1, i).wait_recv()
        span = slice(i * cols, (i + 1) * cols)
        branch = part[half % 2, 0, i] + (
            rs_in[(half - 1) * CHUNKS + i].astype(jnp.float32)
            + rs_in[(2 * half - 1) * CHUNKS + i].astype(jnp.float32)
        )
        out_ref[:, span] = (
            h_ref[:, span].astype(jnp.float32) + mod_ref[2, :, span] * branch
        ).astype(jnp.bfloat16)

    moved = (2 * half - 1) * CHUNKS
    all_sent(rows_all, moved, out_sem.at[0]).wait_send()
    all_sent(kv_own, n, out_sem.at[1]).wait_send()
    all_sent(rs_out, moved, out_sem.at[2]).wait_send()


def local(n, hidden, modulation, qk_gains, counts, offsets, in_weights, out_weights):
    rows, width = hidden.shape[1:]
    head = in_weights.shape[-1]
    half = n // 2
    tokens = n * rows
    cols = width // CHUNKS
    frequency = np.repeat(
        np.exp(np.arange(head // 2, dtype=np.float64) * (-2.0 * math.log(rope_base) / head)), 2
    ).astype(np.float32)[None]
    vmem = pl.BlockSpec(memory_space=pltpu.VMEM)
    anywhere = pl.BlockSpec(memory_space=pl.ANY)
    updated = pl.pallas_call(
        functools.partial(kernel, n),
        out_shape=jax.ShapeDtypeStruct((rows, width), jnp.bfloat16),
        in_specs=[anywhere] * 8,
        out_specs=vmem,
        scratch_shapes=[
            pltpu.VMEM((rows, width), jnp.bfloat16),
            pltpu.VMEM((3, 1, width), jnp.float32),
            pltpu.VMEM((3, 1, head), jnp.float32),
            pltpu.VMEM((1, head), jnp.float32),
            pltpu.SMEM((1, 2), jnp.int32),
            pltpu.SMEM((1, 2), jnp.int32),
            pltpu.VMEM((n * CHUNKS, rows, cols), jnp.bfloat16),
            pltpu.VMEM((width * 4, head), jnp.bfloat16),
            pltpu.VMEM((4 * 128, head), jnp.float32),
            pltpu.VMEM((width, 4 * head), jnp.bfloat16),
            pltpu.VMEM((2 * head, width), jnp.bfloat16),
            pltpu.VMEM((2 * rows, 4 * head), jnp.float32),
            pltpu.VMEM((n, rows, head), jnp.bfloat16),
            pltpu.VMEM((n, rows, head), jnp.bfloat16),
            pltpu.VMEM((n, 2, rows, head), jnp.bfloat16),
            pltpu.VMEM((n, 2, rows, head), jnp.bfloat16),
            pltpu.VMEM((2, tokens), jnp.float32),
            pltpu.VMEM((2, 2 * rows, head), jnp.float32),
            pltpu.VMEM((2 * rows, 2 * head), jnp.bfloat16),
            pltpu.VMEM((2, 2, CHUNKS, rows, cols), jnp.float32),
            pltpu.VMEM((2 * half * CHUNKS, rows, cols), jnp.bfloat16),
            pltpu.VMEM((2 * half * CHUNKS, rows, cols), jnp.bfloat16),
            pltpu.SemaphoreType.DMA((8,)),
            pltpu.SemaphoreType.DMA((3,)),
            pltpu.SemaphoreType.DMA((2, 4, CHUNKS)),
            pltpu.SemaphoreType.DMA,
            pltpu.SemaphoreType.DMA((2, 4, CHUNKS)),
        ],
        compiler_params=pltpu.CompilerParams(
            collective_id=0, has_side_effects=True, vmem_limit_bytes=56 * 1024 * 1024
        ),
    )(
        hidden[0],
        jnp.transpose(modulation, (1, 0, 2)),
        jnp.transpose(qk_gains, (1, 0, 2)),
        jnp.asarray(frequency),
        counts.T,
        offsets.T,
        in_weights.reshape(4 * width, head),
        out_weights.reshape(2 * head, width),
    )
    return updated[None]


def solution(mesh):
    return jax.shard_map(
        functools.partial(local, mesh.shape["tp"]),
        mesh=mesh,
        in_specs=(
            P("tower", ("grp", "tp"), None),
            P("tower", None, None),
            P("tower", None, "tp"),
            P(None, "grp"),
            P(None, "grp"),
            P("tower", None, None, "tp"),
            P("tower", None, "tp", None),
        ),
        out_specs=P("tower", ("grp", "tp"), None),
        check_vma=False,
    )
```

```python
import functools
import math

import jax
import jax.numpy as jnp
import numpy as np
from jax import lax
from jax.experimental import pallas as pl
from jax.experimental.pallas import tpu as pltpu
from jax.sharding import PartitionSpec as P

MESH = pl.DeviceIdType.MESH
epsilon = 1e-06
rope_base = 10000.0
masked_score = -1e30
CHUNKS = 4


def kernel(
    n,
    h_hbm,
    mod_hbm,
    gain_hbm,
    freq_hbm,
    cnt_hbm,
    off_hbm,
    win_hbm,
    wout_hbm,
    out_ref,
    h_ref,
    mod_ref,
    gain_ref,
    freq_ref,
    cnt_ref,
    off_ref,
    rows_all,
    raw,
    wide,
    w_in,
    w_out,
    acc,
    q_all,
    c_all,
    kv_own,
    kv_far,
    bias,
    trig,
    both,
    part,
    rs_in,
    rs_out,
    w_sem,
    out_sem,
    ag_recv,
    kv_recv,
    rs_recv,
):
    half = n // 2
    me = lax.axis_index("tp")
    tower = lax.axis_index("tower")
    right = lax.rem(me + 1, n)
    left = lax.rem(me + n - 1, n)
    other = 1 - tower
    depth = rs_recv.shape[1]
    rows, width = h_ref.shape
    head = gain_ref.shape[-1]
    cols = width // CHUNKS
    tokens = n * rows
    score_scale = math.log2(math.e) / math.sqrt(head)

    loads = [
        pltpu.make_async_copy(source, target, w_sem.at[j])
        for j, (source, target) in enumerate(
            (
                (h_hbm, h_ref),
                (mod_hbm, mod_ref),
                (win_hbm, raw),
                (cnt_hbm, cnt_ref),
                (off_hbm, off_ref),
                (gain_hbm, gain_ref),
                (freq_hbm, freq_ref),
                (wout_hbm, w_out),
            )
        )
    ]
    h_copy, mod_copy, win_copy, cnt_copy, off_copy, gain_copy, freq_copy, wout_copy = loads
    for load in loads:
        load.start()

    barrier = pltpu.get_barrier_semaphore()
    for where in ({"tp": left}, {"tp": right}, {"tower": other}):
        pl.semaphore_signal(barrier, inc=1, device_id=where, device_id_type=MESH)

    def block(offset):
        return lax.rem(me + offset + 2 * n, n)

    def gather_copy(way, step, i):
        piece = block(-step if way == 0 else step) * CHUNKS + i
        return pltpu.make_async_remote_copy(
            src_ref=rows_all.at[piece],
            dst_ref=rows_all.at[piece],
            send_sem=out_sem.at[0],
            recv_sem=ag_recv.at[way, lax.rem(step, depth), i],
            device_id={"tp": right if way == 0 else left},
            device_id_type=MESH,
        )

    def gather_arrival(way, step, i):
        return gather_copy(way, step - 1, i)

    def kv_copy(b):
        return pltpu.make_async_remote_copy(
            src_ref=kv_own.at[b],
            dst_ref=kv_far.at[b],
            send_sem=out_sem.at[1],
            recv_sem=kv_recv,
            device_id={"tower": other},
            device_id_type=MESH,
        )

    def scatter_copy(way, step, i):
        piece = (way * half + step) * CHUNKS + i
        return pltpu.make_async_remote_copy(
            src_ref=rs_out.at[piece],
            dst_ref=rs_in.at[piece],
            send_sem=out_sem.at[2],
            recv_sem=rs_recv.at[way, lax.rem(step, depth), i],
            device_id={"tp": right if way == 0 else left},
            device_id_type=MESH,
        )

    def gather_chunk(way, slot):
        return slot if way == 0 else (slot + CHUNKS // 2) % CHUNKS

    def scatter_chunk(way, slot):
        return gather_chunk(1 - way, slot)

    def all_sent(ref, count, sem):
        return pltpu.make_async_remote_copy(
            src_ref=ref.at[pl.ds(0, count)],
            dst_ref=ref.at[pl.ds(0, count)],
            send_sem=sem,
            recv_sem=kv_recv,
            device_id={"tower": other},
            device_id_type=MESH,
        )

    h_copy.wait()
    mod_copy.wait()
    states = h_ref[...].astype(jnp.float32)
    centre = states - jnp.mean(states, -1, keepdims=True)
    spread = jnp.mean(centre * centre, -1, keepdims=True)
    normed = centre * lax.rsqrt(spread + epsilon) * (1.0 + mod_ref[1]) + mod_ref[0]
    normed = normed.astype(jnp.bfloat16)
    for i in range(CHUNKS):
        rows_all[me * CHUNKS + i] = normed[:, i * cols : (i + 1) * cols]

    pl.semaphore_wait(barrier, 3)
    for slot in range(CHUNKS):
        for way in range(2):
            gather_copy(way, 0, gather_chunk(way, slot)).start()

    cnt_copy.wait()
    key_index = lax.broadcasted_iota(jnp.int32, (1, tokens), 1)
    bias[0:1, :] = jnp.where(key_index < cnt_ref[0, tower], 0.0, masked_score)
    bias[1:2, :] = jnp.where(key_index < cnt_ref[0, other], 0.0, masked_score)

    win_copy.wait()
    fold = wide.shape[0] // 4

    def unfold(j, carry):
        wide[...] = raw[pl.ds(pl.multiple_of(j * 4 * fold, 4 * fold), 4 * fold), :].astype(jnp.float32)
        for c in range(4):
            w_in[pl.ds(pl.multiple_of(j * fold, fold), fold), c * head : (c + 1) * head] = wide[
                pl.ds(c, fold, stride=4), :
            ].astype(jnp.bfloat16)
        return carry

    lax.fori_loop(0, width // fold, unfold, 0)
    for load in (off_copy, gain_copy, freq_copy, wout_copy):
        load.wait()

    lane = lax.broadcasted_iota(jnp.int32, (1, head), 1)
    is_even = lax.rem(lane, 2) == 0
    offset = off_ref[0, tower]

    def row_positions(b):
        return offset + b * rows + lax.broadcasted_iota(jnp.int32, (rows, 1), 0)

    def project(i, blocks, first):
        picked = [rows_all[b * CHUNKS + i] for b in blocks]
        lhs = picked[0] if len(picked) == 1 else jnp.concatenate(picked, 0)
        term = jnp.dot(lhs, w_in[i * cols : (i + 1) * cols, :], preferred_element_type=jnp.float32)
        if first:
            acc[: lhs.shape[0], :] = term
        else:
            acc[: lhs.shape[0], :] += term

    def prepare_turn(blocks):
        for j, b in enumerate(blocks):
            angles = row_positions(b).astype(jnp.float32) * freq_ref[...]
            sine = jnp.sin(angles)
            trig[0, j * rows : (j + 1) * rows] = jnp.cos(angles)
            trig[1, j * rows : (j + 1) * rows] = jnp.where(is_even, -sine, sine)

    def finish(blocks, send=False):
        count = len(blocks) * rows
        cosine = trig[0, :count]
        sine = trig[1, :count]

        def turned(c, g):
            x = acc[:count, c * head : (c + 1) * head]
            square = jnp.mean(x * x, -1, keepdims=True)
            x = x * lax.rsqrt(square + epsilon) * gain_ref[g]
            swapped = jnp.where(is_even, pltpu.roll(x, head - 1, 1), pltpu.roll(x, 1, 1))
            return (x * cosine + swapped * sine).astype(jnp.bfloat16)

        keys = turned(1, 1)
        values = acc[:count, 2 * head : 3 * head].astype(jnp.bfloat16)
        for j, b in enumerate(blocks):
            span = slice(j * rows, (j + 1) * rows)
            kv_own[b, 0] = keys[span]
            kv_own[b, 1] = values[span]
            if send:
                kv_copy(b).start()
        queries = turned(0, 0)
        cross = turned(3, 2)
        for j, b in enumerate(blocks):
            span = slice(j * rows, (j + 1) * rows)
            q_all[b] = queries[span]
            c_all[b] = cross[span]

    for i in range(CHUNKS):
        project(i, [me], i == 0)
    prepare_turn([me])
    finish([me])

    def gather_step(step, carry):
        before, after = block(-step), block(step)
        prepare_turn([before, after])
        for slot in range(CHUNKS):
            for way in range(2):
                i = gather_chunk(way, slot)
                gather_arrival(way, step, i).wait_recv()
                if slot < CHUNKS // 2:
                    gather_copy(way, step, i).start()
                else:
                    pl.when(step < half - 1)(lambda way=way, i=i: gather_copy(way, step, i).start())
            if slot == 0:
                kv_copy(block(1 - step)).start()
                pl.when(step > 1)(lambda: kv_copy(block(step - 1)).start())
            if slot >= CHUNKS // 2:
                project(gather_chunk(0, slot), [before, after], slot == CHUNKS // 2)
                project(gather_chunk(1, slot), [before, after], False)
        finish([before, after])
        return carry

    lax.fori_loop(1, half, gather_step, 0)
    kv_copy(block(1 - half)).start()
    kv_copy(block(half - 1)).start()
    last = block(half)
    prepare_turn([last])
    quiet = jnp.zeros((rows, cols), jnp.bfloat16)
    for i in range(CHUNKS):
        rs_in[(half if i < CHUNKS // 2 else 0) * CHUNKS + i] = quiet
    for slot in range(CHUNKS // 2):
        for way in range(2):
            i = gather_chunk(way, slot)
            gather_arrival(way, half, i).wait_recv()
            project(i, [last], slot == 0 and way == 0)
    finish([last], True)

    def attend(queries, pairs, row):
        keys = pairs[:, 0].reshape(tokens, head)
        values = pairs[:, 1].reshape(tokens, head)
        scores = lax.dot_general(
            queries, keys, (((1,), (1,)), ((), ())), preferred_element_type=jnp.float32
        )
        scores = scores * score_scale + bias[row : row + 1, :]
        raised = jnp.exp2(scores - jnp.max(scores, -1, keepdims=True))
        total = jnp.sum(raised, -1, keepdims=True)
        summed = jnp.dot(raised.astype(jnp.bfloat16), values, preferred_element_type=jnp.float32)
        return (summed / total).astype(jnp.bfloat16)

    def attend_self(blocks):
        picked = [q_all[b] for b in blocks]
        lhs = picked[0] if len(picked) == 1 else jnp.concatenate(picked, 0)
        both[: lhs.shape[0], :head] = attend(lhs, kv_own, 0)

    def attend_cross(blocks):
        picked = [c_all[b] for b in blocks]
        lhs = picked[0] if len(picked) == 1 else jnp.concatenate(picked, 0)
        both[: lhs.shape[0], head:] = attend(lhs, kv_far, 1)

    def expand(count, i):
        return jnp.dot(
            both[:count, :], w_out[:, i * cols : (i + 1) * cols], preferred_element_type=jnp.float32
        )

    def partial_piece(turn, blocks, piece):
        if piece == 0:
            attend_self(blocks)
        elif piece == 1:
            attend_cross(blocks)
        else:
            for i in range(2 * (piece - 2), 2 * (piece - 1)):
                term = expand(2 * rows, i)
                part[turn, 0, i] = term[:rows]
                part[turn, 1, i] = term[rows:]

    attend_self([last])
    pltpu.make_async_copy(kv_far, kv_far, kv_recv).wait()
    attend_cross([last])
    for i in (0, 2, 1, 3):
        way = 0 if i < CHUNKS // 2 else 1
        rs_out[way * half * CHUNKS + i] = expand(rows, i).astype(jnp.bfloat16)
        scatter_copy(way, 0, i).start()
    for piece in range(4):
        partial_piece(1, [block(half - 1), block(1 - half)], piece)

    def scatter_step(step, carry):
        turn = lax.rem(step, 2)
        following = [block(half - 1 - step), block(step + 1 - half)]
        for slot in range(CHUNKS):
            for way in range(2):
                i = scatter_chunk(way, slot)
                if slot >= CHUNKS // 2:
                    scatter_copy(way, step - 1, i).wait_recv()
                else:
                    pl.when(step > 1)(lambda way=way, i=i: scatter_copy(way, step - 1, i).wait_recv())
                running = rs_in[(way * half + step - 1) * CHUNKS + i].astype(jnp.float32) + part[turn, way, i]
                rs_out[(way * half + step) * CHUNKS + i] = running.astype(jnp.bfloat16)
                scatter_copy(way, step, i).start()
            partial_piece(1 - turn, following, slot)
        return carry

    lax.fori_loop(1, half, scatter_step, 0)
    for i in (0, 2, 1, 3):
        scatter_copy(0, half - 1, i).wait_recv()
        scatter_copy(1, half - 1, i).wait_recv()
        span = slice(i * cols, (i + 1) * cols)
        branch = part[half % 2, 0, i] + (
            rs_in[(half - 1) * CHUNKS + i].astype(jnp.float32)
            + rs_in[(2 * half - 1) * CHUNKS + i].astype(jnp.float32)
        )
        out_ref[:, span] = (
            h_ref[:, span].astype(jnp.float32) + mod_ref[2, :, span] * branch
        ).astype(jnp.bfloat16)

    moved = (2 * half - 1) * CHUNKS
    all_sent(rows_all, moved, out_sem.at[0]).wait_send()
    all_sent(kv_own, n, out_sem.at[1]).wait_send()
    all_sent(rs_out, moved, out_sem.at[2]).wait_send()


def local(n, hidden, modulation, qk_gains, counts, offsets, in_weights, out_weights):
    rows, width = hidden.shape[1:]
    head = in_weights.shape[-1]
    half = n // 2
    tokens = n * rows
    cols = width // CHUNKS
    frequency = np.repeat(
        np.exp(np.arange(head // 2, dtype=np.float64) * (-2.0 * math.log(rope_base) / head)), 2
    ).astype(np.float32)[None]
    vmem = pl.BlockSpec(memory_space=pltpu.VMEM)
    anywhere = pl.BlockSpec(memory_space=pl.ANY)
    updated = pl.pallas_call(
        functools.partial(kernel, n),
        out_shape=pltpu.VMEM((rows, width), jnp.bfloat16),
        in_specs=[anywhere] * 8,
        out_specs=vmem,
        scratch_shapes=[
            pltpu.VMEM((rows, width), jnp.bfloat16),
            pltpu.VMEM((3, 1, width), jnp.float32),
            pltpu.VMEM((3, 1, head), jnp.float32),
            pltpu.VMEM((1, head), jnp.float32),
            pltpu.SMEM((1, 2), jnp.int32),
            pltpu.SMEM((1, 2), jnp.int32),
            pltpu.VMEM((n * CHUNKS, rows, cols), jnp.bfloat16),
            pltpu.VMEM((width * 4, head), jnp.bfloat16),
            pltpu.VMEM((4 * 128, head), jnp.float32),
            pltpu.VMEM((width, 4 * head), jnp.bfloat16),
            pltpu.VMEM((2 * head, width), jnp.bfloat16),
            pltpu.VMEM((2 * rows, 4 * head), jnp.float32),
            pltpu.VMEM((n, rows, head), jnp.bfloat16),
            pltpu.VMEM((n, rows, head), jnp.bfloat16),
            pltpu.VMEM((n, 2, rows, head), jnp.bfloat16),
            pltpu.VMEM((n, 2, rows, head), jnp.bfloat16),
            pltpu.VMEM((2, tokens), jnp.float32),
            pltpu.VMEM((2, 2 * rows, head), jnp.float32),
            pltpu.VMEM((2 * rows, 2 * head), jnp.bfloat16),
            pltpu.VMEM((2, 2, CHUNKS, rows, cols), jnp.float32),
            pltpu.VMEM((2 * half * CHUNKS, rows, cols), jnp.bfloat16),
            pltpu.VMEM((2 * half * CHUNKS, rows, cols), jnp.bfloat16),
            pltpu.SemaphoreType.DMA((8,)),
            pltpu.SemaphoreType.DMA((3,)),
            pltpu.SemaphoreType.DMA((2, 4, CHUNKS)),
            pltpu.SemaphoreType.DMA,
            pltpu.SemaphoreType.DMA((2, 4, CHUNKS)),
        ],
        compiler_params=pltpu.CompilerParams(
            collective_id=0, has_side_effects=True, vmem_limit_bytes=56 * 1024 * 1024
        ),
    )(
        hidden[0],
        jnp.transpose(modulation, (1, 0, 2)),
        jnp.transpose(qk_gains, (1, 0, 2)),
        jnp.asarray(frequency),
        counts.T,
        offsets.T,
        in_weights.reshape(4 * width, head),
        out_weights.reshape(2 * head, width),
    )
    return updated[None]


def solution(mesh):
    return jax.shard_map(
        functools.partial(local, mesh.shape["tp"]),
        mesh=mesh,
        in_specs=(
            P("tower", ("grp", "tp"), None),
            P("tower", None, None),
            P("tower", None, "tp"),
            P(None, "grp"),
            P(None, "grp"),
            P("tower", None, None, "tp"),
            P("tower", None, "tp", None),
        ),
        out_specs=P("tower", ("grp", "tp"), None),
        check_vma=False,
    )
```

```python
import functools
import math

import jax
import jax.numpy as jnp
import numpy as np
from jax import lax
from jax.experimental import pallas as pl
from jax.experimental.pallas import tpu as pltpu
from jax.sharding import PartitionSpec as P

MESH = pl.DeviceIdType.MESH
epsilon = 1e-06
rope_base = 10000.0
masked_score = -1e30
CHUNKS = 4


def kernel(
    n,
    h_hbm,
    mod_hbm,
    gain_hbm,
    freq_hbm,
    cnt_hbm,
    off_hbm,
    win_hbm,
    wout_hbm,
    out_ref,
    h_ref,
    mod_ref,
    gain_ref,
    freq_ref,
    cnt_ref,
    off_ref,
    rows_all,
    raw,
    wide,
    w_in,
    w_out,
    acc,
    q_all,
    c_all,
    kv_own,
    kv_far,
    bias,
    trig,
    both,
    part,
    rs_in,
    rs_out,
    w_sem,
    out_sem,
    recv,
    kv_recv,
):
    half = n // 2
    me = lax.axis_index("tp")
    tower = lax.axis_index("tower")
    right = lax.rem(me + 1, n)
    left = lax.rem(me + n - 1, n)
    other = 1 - tower
    depth = recv.shape[1]
    rows, width = h_ref.shape
    head = gain_ref.shape[-1]
    cols = width // CHUNKS
    tokens = n * rows
    score_scale = math.log2(math.e) / math.sqrt(head)

    loads = [
        pltpu.make_async_copy(source, target, w_sem.at[j])
        for j, (source, target) in enumerate(
            (
                (h_hbm, h_ref),
                (mod_hbm, mod_ref),
                (win_hbm, raw),
                (cnt_hbm, cnt_ref),
                (off_hbm, off_ref),
                (gain_hbm, gain_ref),
                (freq_hbm, freq_ref),
                (wout_hbm, w_out),
            )
        )
    ]
    h_copy, mod_copy, win_copy, cnt_copy, off_copy, gain_copy, freq_copy, wout_copy = loads
    for load in loads:
        load.start()

    barrier = pltpu.get_barrier_semaphore()
    for where in ({"tp": left}, {"tp": right}, {"tower": other}):
        pl.semaphore_signal(barrier, inc=1, device_id=where, device_id_type=MESH)

    def block(offset):
        return lax.rem(me + offset + 2 * n, n)

    def gather_copy(way, step, i):
        piece = block(-step if way == 0 else step) * CHUNKS + i
        return pltpu.make_async_remote_copy(
            src_ref=rows_all.at[piece],
            dst_ref=rows_all.at[piece],
            send_sem=out_sem.at[0],
            recv_sem=recv.at[way, lax.rem(step, depth), i],
            device_id={"tp": right if way == 0 else left},
            device_id_type=MESH,
        )

    def gather_arrival(way, step, i):
        return gather_copy(way, step - 1, i)

    def kv_copy(b):
        return pltpu.make_async_remote_copy(
            src_ref=kv_own.at[b],
            dst_ref=kv_far.at[b],
            send_sem=out_sem.at[1],
            recv_sem=kv_recv,
            device_id={"tower": other},
            device_id_type=MESH,
        )

    def scatter_copy(way, step, i):
        piece = (way * half + step) * CHUNKS + i
        return pltpu.make_async_remote_copy(
            src_ref=rs_out.at[piece],
            dst_ref=rs_in.at[piece],
            send_sem=out_sem.at[2],
            recv_sem=recv.at[way, lax.rem(step, depth), i],
            device_id={"tp": right if way == 0 else left},
            device_id_type=MESH,
        )

    def gather_chunk(way, slot):
        return slot if way == 0 else (slot + CHUNKS // 2) % CHUNKS

    def scatter_chunk(way, slot):
        return gather_chunk(1 - way, slot)

    def all_sent(ref, count, sem):
        return pltpu.make_async_remote_copy(
            src_ref=ref.at[pl.ds(0, count)],
            dst_ref=ref.at[pl.ds(0, count)],
            send_sem=sem,
            recv_sem=kv_recv,
            device_id={"tower": other},
            device_id_type=MESH,
        )

    h_copy.wait()
    mod_copy.wait()
    states = h_ref[...].astype(jnp.float32)
    centre = states - jnp.mean(states, -1, keepdims=True)
    spread = jnp.mean(centre * centre, -1, keepdims=True)
    normed = centre * lax.rsqrt(spread + epsilon) * (1.0 + mod_ref[1]) + mod_ref[0]
    normed = normed.astype(jnp.bfloat16)
    for i in range(CHUNKS):
        rows_all[me * CHUNKS + i] = normed[:, i * cols : (i + 1) * cols]

    pl.semaphore_wait(barrier, 3)
    for slot in range(CHUNKS):
        for way in range(2):
            gather_copy(way, 0, gather_chunk(way, slot)).start()

    cnt_copy.wait()
    key_index = lax.broadcasted_iota(jnp.int32, (1, tokens), 1)
    bias[0:1, :] = jnp.where(key_index < cnt_ref[0, tower], 0.0, masked_score)
    bias[1:2, :] = jnp.where(key_index < cnt_ref[0, other], 0.0, masked_score)

    win_copy.wait()
    fold = wide.shape[0] // 4

    def unfold(j, carry):
        wide[...] = raw[pl.ds(pl.multiple_of(j * 4 * fold, 4 * fold), 4 * fold), :].astype(jnp.float32)
        for c in range(4):
            w_in[pl.ds(pl.multiple_of(j * fold, fold), fold), c * head : (c + 1) * head] = wide[
                pl.ds(c, fold, stride=4), :
            ].astype(jnp.bfloat16)
        return carry

    lax.fori_loop(0, width // fold, unfold, 0)
    for load in (off_copy, gain_copy, freq_copy, wout_copy):
        load.wait()

    lane = lax.broadcasted_iota(jnp.int32, (1, head), 1)
    is_even = lax.rem(lane, 2) == 0
    offset = off_ref[0, tower]

    def row_positions(b):
        return offset + b * rows + lax.broadcasted_iota(jnp.int32, (rows, 1), 0)

    def project(i, blocks, first):
        picked = [rows_all[b * CHUNKS + i] for b in blocks]
        lhs = picked[0] if len(picked) == 1 else jnp.concatenate(picked, 0)
        term = jnp.dot(lhs, w_in[i * cols : (i + 1) * cols, :], preferred_element_type=jnp.float32)
        if first:
            acc[: lhs.shape[0], :] = term
        else:
            acc[: lhs.shape[0], :] += term

    def prepare_turn(blocks):
        for j, b in enumerate(blocks):
            angles = row_positions(b).astype(jnp.float32) * freq_ref[...]
            sine = jnp.sin(angles)
            trig[0, j * rows : (j + 1) * rows] = jnp.cos(angles)
            trig[1, j * rows : (j + 1) * rows] = jnp.where(is_even, -sine, sine)

    def finish(blocks, send=False):
        count = len(blocks) * rows
        cosine = trig[0, :count]
        sine = trig[1, :count]

        def turned(c, g):
            x = acc[:count, c * head : (c + 1) * head]
            square = jnp.mean(x * x, -1, keepdims=True)
            x = x * lax.rsqrt(square + epsilon) * gain_ref[g]
            swapped = jnp.where(is_even, pltpu.roll(x, head - 1, 1), pltpu.roll(x, 1, 1))
            return (x * cosine + swapped * sine).astype(jnp.bfloat16)

        keys = turned(1, 1)
        values = acc[:count, 2 * head : 3 * head].astype(jnp.bfloat16)
        for j, b in enumerate(blocks):
            span = slice(j * rows, (j + 1) * rows)
            kv_own[b, 0] = keys[span]
            kv_own[b, 1] = values[span]
            if send:
                kv_copy(b).start()
        queries = turned(0, 0)
        cross = turned(3, 2)
        for j, b in enumerate(blocks):
            span = slice(j * rows, (j + 1) * rows)
            q_all[b] = queries[span]
            c_all[b] = cross[span]

    for i in range(CHUNKS):
        project(i, [me], i == 0)
    prepare_turn([me])
    finish([me])

    def gather_step(step, carry):
        before, after = block(-step), block(step)
        prepare_turn([before, after])
        for slot in range(CHUNKS):
            for way in range(2):
                i = gather_chunk(way, slot)
                gather_arrival(way, step, i).wait_recv()
                if slot < CHUNKS // 2:
                    gather_copy(way, step, i).start()
                else:
                    pl.when(step < half - 1)(lambda way=way, i=i: gather_copy(way, step, i).start())
            if slot == 0:
                kv_copy(block(1 - step)).start()
                pl.when(step > 1)(lambda: kv_copy(block(step - 1)).start())
            if slot >= CHUNKS // 2:
                project(gather_chunk(0, slot), [before, after], slot == CHUNKS // 2)
                project(gather_chunk(1, slot), [before, after], False)
        finish([before, after])
        return carry

    lax.fori_loop(1, half, gather_step, 0)
    kv_copy(block(1 - half)).start()
    kv_copy(block(half - 1)).start()
    last = block(half)
    prepare_turn([last])
    quiet = jnp.zeros((rows, cols), jnp.bfloat16)
    for i in range(CHUNKS):
        rs_in[(half if i < CHUNKS // 2 else 0) * CHUNKS + i] = quiet
    for slot in range(CHUNKS // 2):
        for way in range(2):
            i = gather_chunk(way, slot)
            gather_arrival(way, half, i).wait_recv()
            project(i, [last], slot == 0 and way == 0)
    finish([last], True)

    def attend(queries, pairs, row):
        keys = pairs[:, 0].reshape(tokens, head)
        values = pairs[:, 1].reshape(tokens, head)
        scores = lax.dot_general(
            queries, keys, (((1,), (1,)), ((), ())), preferred_element_type=jnp.float32
        )
        scores = scores * score_scale + bias[row : row + 1, :]
        raised = jnp.exp2(scores - jnp.max(scores, -1, keepdims=True))
        total = jnp.sum(raised, -1, keepdims=True)
        summed = jnp.dot(raised.astype(jnp.bfloat16), values, preferred_element_type=jnp.float32)
        return (summed / total).astype(jnp.bfloat16)

    def attend_self(blocks):
        picked = [q_all[b] for b in blocks]
        lhs = picked[0] if len(picked) == 1 else jnp.concatenate(picked, 0)
        both[: lhs.shape[0], :head] = attend(lhs, kv_own, 0)

    def attend_cross(blocks):
        picked = [c_all[b] for b in blocks]
        lhs = picked[0] if len(picked) == 1 else jnp.concatenate(picked, 0)
        both[: lhs.shape[0], head:] = attend(lhs, kv_far, 1)

    def expand(count, i):
        return jnp.dot(
            both[:count, :], w_out[:, i * cols : (i + 1) * cols], preferred_element_type=jnp.float32
        )

    def partial_piece(turn, blocks, piece):
        if piece == 0:
            attend_self(blocks)
        elif piece == 1:
            attend_cross(blocks)
        else:
            for i in range(2 * (piece - 2), 2 * (piece - 1)):
                term = expand(2 * rows, i)
                part[turn, 0, i] = term[:rows]
                part[turn, 1, i] = term[rows:]

    attend_self([last])
    for i in range(CHUNKS):
        part[0, 0, i] = jnp.dot(
            both[:rows, :head],
            w_out[:head, i * cols : (i + 1) * cols],
            preferred_element_type=jnp.float32,
        )
    pltpu.make_async_copy(kv_far, kv_far, kv_recv).wait()
    attend_cross([last])
    for i in (0, 2, 1, 3):
        way = 0 if i < CHUNKS // 2 else 1
        term = part[0, 0, i] + jnp.dot(
            both[:rows, head:],
            w_out[head:, i * cols : (i + 1) * cols],
            preferred_element_type=jnp.float32,
        )
        rs_out[way * half * CHUNKS + i] = term.astype(jnp.bfloat16)
        scatter_copy(way, 0, i).start()
    for piece in range(4):
        partial_piece(1, [block(half - 1), block(1 - half)], piece)

    def scatter_step(step, carry):
        turn = lax.rem(step, 2)
        following = [block(half - 1 - step), block(step + 1 - half)]
        for slot in range(CHUNKS):
            for way in range(2):
                i = scatter_chunk(way, slot)
                if slot >= CHUNKS // 2:
                    scatter_copy(way, step - 1, i).wait_recv()
                else:
                    pl.when(step > 1)(lambda way=way, i=i: scatter_copy(way, step - 1, i).wait_recv())
                running = rs_in[(way * half + step - 1) * CHUNKS + i].astype(jnp.float32) + part[turn, way, i]
                rs_out[(way * half + step) * CHUNKS + i] = running.astype(jnp.bfloat16)
                scatter_copy(way, step, i).start()
            partial_piece(1 - turn, following, slot)
        return carry

    lax.fori_loop(1, half, scatter_step, 0)
    for i in (0, 2, 1, 3):
        scatter_copy(0, half - 1, i).wait_recv()
        scatter_copy(1, half - 1, i).wait_recv()
        span = slice(i * cols, (i + 1) * cols)
        branch = part[half % 2, 0, i] + (
            rs_in[(half - 1) * CHUNKS + i].astype(jnp.float32)
            + rs_in[(2 * half - 1) * CHUNKS + i].astype(jnp.float32)
        )
        out_ref[:, span] = (
            h_ref[:, span].astype(jnp.float32) + mod_ref[2, :, span] * branch
        ).astype(jnp.bfloat16)

    moved = (2 * half - 1) * CHUNKS
    all_sent(rows_all, moved, out_sem.at[0]).wait_send()
    all_sent(kv_own, n, out_sem.at[1]).wait_send()
    all_sent(rs_out, moved, out_sem.at[2]).wait_send()


def local(n, hidden, modulation, qk_gains, counts, offsets, in_weights, out_weights):
    rows, width = hidden.shape[1:]
    head = in_weights.shape[-1]
    half = n // 2
    tokens = n * rows
    cols = width // CHUNKS
    frequency = np.repeat(
        np.exp(np.arange(head // 2, dtype=np.float64) * (-2.0 * math.log(rope_base) / head)), 2
    ).astype(np.float32)[None]
    vmem = pl.BlockSpec(memory_space=pltpu.VMEM)
    anywhere = pl.BlockSpec(memory_space=pl.ANY)
    updated = pl.pallas_call(
        functools.partial(kernel, n),
        out_shape=pltpu.VMEM((rows, width), jnp.bfloat16),
        in_specs=[anywhere] * 8,
        out_specs=vmem,
        scratch_shapes=[
            pltpu.VMEM((rows, width), jnp.bfloat16),
            pltpu.VMEM((3, 1, width), jnp.float32),
            pltpu.VMEM((3, 1, head), jnp.float32),
            pltpu.VMEM((1, head), jnp.float32),
            pltpu.SMEM((1, 2), jnp.int32),
            pltpu.SMEM((1, 2), jnp.int32),
            pltpu.VMEM((n * CHUNKS, rows, cols), jnp.bfloat16),
            pltpu.VMEM((width * 4, head), jnp.bfloat16),
            pltpu.VMEM((4 * 128, head), jnp.float32),
            pltpu.VMEM((width, 4 * head), jnp.bfloat16),
            pltpu.VMEM((2 * head, width), jnp.bfloat16),
            pltpu.VMEM((2 * rows, 4 * head), jnp.float32),
            pltpu.VMEM((n, rows, head), jnp.bfloat16),
            pltpu.VMEM((n, rows, head), jnp.bfloat16),
            pltpu.VMEM((n, 2, rows, head), jnp.bfloat16),
            pltpu.VMEM((n, 2, rows, head), jnp.bfloat16),
            pltpu.VMEM((2, tokens), jnp.float32),
            pltpu.VMEM((2, 2 * rows, head), jnp.float32),
            pltpu.VMEM((2 * rows, 2 * head), jnp.bfloat16),
            pltpu.VMEM((2, 2, CHUNKS, rows, cols), jnp.float32),
            pltpu.VMEM((2 * half * CHUNKS, rows, cols), jnp.bfloat16),
            pltpu.VMEM((2 * half * CHUNKS, rows, cols), jnp.bfloat16),
            pltpu.SemaphoreType.DMA((8,)),
            pltpu.SemaphoreType.DMA((3,)),
            pltpu.SemaphoreType.DMA((2, 4, CHUNKS)),
            pltpu.SemaphoreType.DMA,
        ],
        compiler_params=pltpu.CompilerParams(
            collective_id=0, has_side_effects=True, vmem_limit_bytes=56 * 1024 * 1024
        ),
    )(
        hidden[0],
        jnp.transpose(modulation, (1, 0, 2)),
        jnp.transpose(qk_gains, (1, 0, 2)),
        jnp.asarray(frequency),
        counts.T,
        offsets.T,
        in_weights.reshape(4 * width, head),
        out_weights.reshape(2 * head, width),
    )
    return updated[None]


def solution(mesh):
    return jax.shard_map(
        functools.partial(local, mesh.shape["tp"]),
        mesh=mesh,
        in_specs=(
            P("tower", ("grp", "tp"), None),
            P("tower", None, None),
            P("tower", None, "tp"),
            P(None, "grp"),
            P(None, "grp"),
            P("tower", None, None, "tp"),
            P("tower", None, "tp", None),
        ),
        out_specs=P("tower", ("grp", "tp"), None),
        check_vma=False,
    )
```

```python
import functools
import math

import jax
import jax.numpy as jnp
import numpy as np
from jax import lax
from jax.experimental import pallas as pl
from jax.experimental.pallas import tpu as pltpu
from jax.sharding import PartitionSpec as P

MESH = pl.DeviceIdType.MESH
epsilon = 1e-06
rope_base = 10000.0
masked_score = -1e30
CHUNKS = 4


def kernel(
    n,
    h_hbm,
    mod_hbm,
    gain_hbm,
    freq_hbm,
    cnt_hbm,
    off_hbm,
    win_hbm,
    wout_hbm,
    out_ref,
    h_ref,
    mod_ref,
    gain_ref,
    freq_ref,
    cnt_ref,
    off_ref,
    rows_all,
    raw,
    wide,
    w_in,
    w_out,
    acc,
    q_all,
    c_all,
    kv_own,
    kv_far,
    bias,
    trig,
    both,
    part,
    rs_in,
    rs_out,
    w_sem,
    out_sem,
    recv,
    kv_recv,
):
    half = n // 2
    me = lax.axis_index("tp")
    tower = lax.axis_index("tower")
    right = lax.rem(me + 1, n)
    left = lax.rem(me + n - 1, n)
    other = 1 - tower
    depth = recv.shape[1]
    rows, width = h_ref.shape
    head = gain_ref.shape[-1]
    cols = width // CHUNKS
    tokens = n * rows
    score_scale = math.log2(math.e) / math.sqrt(head)

    loads = [
        pltpu.make_async_copy(source, target, w_sem.at[j])
        for j, (source, target) in enumerate(
            (
                (h_hbm, h_ref),
                (mod_hbm, mod_ref),
                (win_hbm, raw),
                (cnt_hbm, cnt_ref),
                (off_hbm, off_ref),
                (gain_hbm, gain_ref),
                (freq_hbm, freq_ref),
                (wout_hbm, w_out),
            )
        )
    ]
    h_copy, mod_copy, win_copy, cnt_copy, off_copy, gain_copy, freq_copy, wout_copy = loads
    for load in loads:
        load.start()

    barrier = pltpu.get_barrier_semaphore()
    for where in ({"tp": left}, {"tp": right}, {"tower": other}):
        pl.semaphore_signal(barrier, inc=1, device_id=where, device_id_type=MESH)

    def block(offset):
        return lax.rem(me + offset + 2 * n, n)

    def gather_copy(way, step, i):
        piece = block(-step if way == 0 else step) * CHUNKS + i
        return pltpu.make_async_remote_copy(
            src_ref=rows_all.at[piece],
            dst_ref=rows_all.at[piece],
            send_sem=out_sem.at[0],
            recv_sem=recv.at[way, lax.rem(step, depth), i],
            device_id={"tp": right if way == 0 else left},
            device_id_type=MESH,
        )

    def gather_arrival(way, step, i):
        return gather_copy(way, step - 1, i)

    def kv_copy(b):
        return pltpu.make_async_remote_copy(
            src_ref=kv_own.at[b],
            dst_ref=kv_far.at[b],
            send_sem=out_sem.at[1],
            recv_sem=kv_recv,
            device_id={"tower": other},
            device_id_type=MESH,
        )

    def scatter_copy(way, step, i):
        piece = (way * half + step) * CHUNKS + i
        return pltpu.make_async_remote_copy(
            src_ref=rs_out.at[piece],
            dst_ref=rs_in.at[piece],
            send_sem=out_sem.at[2],
            recv_sem=recv.at[way, lax.rem(step, depth), i],
            device_id={"tp": right if way == 0 else left},
            device_id_type=MESH,
        )

    def gather_chunk(way, slot):
        return slot if way == 0 else (slot + CHUNKS // 2) % CHUNKS

    def scatter_chunk(way, slot):
        return gather_chunk(1 - way, slot)

    def all_sent(ref, count, sem):
        return pltpu.make_async_remote_copy(
            src_ref=ref.at[pl.ds(0, count)],
            dst_ref=ref.at[pl.ds(0, count)],
            send_sem=sem,
            recv_sem=kv_recv,
            device_id={"tower": other},
            device_id_type=MESH,
        )

    h_copy.wait()
    mod_copy.wait()
    states = h_ref[...].astype(jnp.float32)
    centre = states - jnp.mean(states, -1, keepdims=True)
    spread = jnp.mean(centre * centre, -1, keepdims=True)
    normed = centre * lax.rsqrt(spread + epsilon) * (1.0 + mod_ref[1]) + mod_ref[0]
    normed = normed.astype(jnp.bfloat16)
    for i in range(CHUNKS):
        rows_all[me * CHUNKS + i] = normed[:, i * cols : (i + 1) * cols]

    pl.semaphore_wait(barrier, 3)
    for slot in range(CHUNKS):
        for way in range(2):
            gather_copy(way, 0, gather_chunk(way, slot)).start()

    cnt_copy.wait()
    key_index = lax.broadcasted_iota(jnp.int32, (1, tokens), 1)
    bias[0:1, :] = jnp.where(key_index < cnt_ref[0, tower], 0.0, masked_score)
    bias[1:2, :] = jnp.where(key_index < cnt_ref[0, other], 0.0, masked_score)

    win_copy.wait()
    fold = wide.shape[0] // 4
    placed = (1, 2, 0, 3)

    def unfold(j, carry):
        wide[...] = raw[pl.ds(pl.multiple_of(j * 4 * fold, 4 * fold), 4 * fold), :].astype(jnp.float32)
        for place, c in enumerate(placed):
            w_in[pl.ds(pl.multiple_of(j * fold, fold), fold), place * head : (place + 1) * head] = wide[
                pl.ds(c, fold, stride=4), :
            ].astype(jnp.bfloat16)
        return carry

    lax.fori_loop(0, width // fold, unfold, 0)
    for load in (off_copy, gain_copy, freq_copy, wout_copy):
        load.wait()

    lane = lax.broadcasted_iota(jnp.int32, (1, head), 1)
    is_even = lax.rem(lane, 2) == 0
    offset = off_ref[0, tower]

    def row_positions(b):
        return offset + b * rows + lax.broadcasted_iota(jnp.int32, (rows, 1), 0)

    def project(i, blocks, first, begin=0, end=4):
        picked = [rows_all[b * CHUNKS + i] for b in blocks]
        lhs = picked[0] if len(picked) == 1 else jnp.concatenate(picked, 0)
        span = slice(begin * head, end * head)
        term = jnp.dot(lhs, w_in[i * cols : (i + 1) * cols, span], preferred_element_type=jnp.float32)
        if first:
            acc[: lhs.shape[0], span] = term
        else:
            acc[: lhs.shape[0], span] += term

    def prepare_turn(blocks):
        for j, b in enumerate(blocks):
            angles = row_positions(b).astype(jnp.float32) * freq_ref[...]
            sine = jnp.sin(angles)
            trig[0, j * rows : (j + 1) * rows] = jnp.cos(angles)
            trig[1, j * rows : (j + 1) * rows] = jnp.where(is_even, -sine, sine)

    def turned(count, place, g):
        x = acc[:count, place * head : (place + 1) * head]
        square = jnp.mean(x * x, -1, keepdims=True)
        x = x * lax.rsqrt(square + epsilon) * gain_ref[g]
        swapped = jnp.where(is_even, pltpu.roll(x, head - 1, 1), pltpu.roll(x, 1, 1))
        return (x * trig[0, :count] + swapped * trig[1, :count]).astype(jnp.bfloat16)

    def finish_pairs(blocks):
        count = len(blocks) * rows
        keys = turned(count, 0, 1)
        values = acc[:count, head : 2 * head].astype(jnp.bfloat16)
        for j, b in enumerate(blocks):
            span = slice(j * rows, (j + 1) * rows)
            kv_own[b, 0] = keys[span]
            kv_own[b, 1] = values[span]

    def finish_queries(blocks):
        count = len(blocks) * rows
        queries = turned(count, 2, 0)
        cross = turned(count, 3, 2)
        for j, b in enumerate(blocks):
            span = slice(j * rows, (j + 1) * rows)
            q_all[b] = queries[span]
            c_all[b] = cross[span]

    def finish(blocks):
        finish_pairs(blocks)
        finish_queries(blocks)

    for i in range(CHUNKS):
        project(i, [me], i == 0)
    prepare_turn([me])
    finish([me])

    def gather_step(step, carry):
        before, after = block(-step), block(step)
        prepare_turn([before, after])
        for slot in range(CHUNKS):
            for way in range(2):
                i = gather_chunk(way, slot)
                gather_arrival(way, step, i).wait_recv()
                if slot < CHUNKS // 2:
                    gather_copy(way, step, i).start()
                else:
                    pl.when(step < half - 1)(lambda way=way, i=i: gather_copy(way, step, i).start())
            if slot == 0:
                kv_copy(block(1 - step)).start()
                pl.when(step > 1)(lambda: kv_copy(block(step - 1)).start())
            if slot >= CHUNKS // 2:
                project(gather_chunk(0, slot), [before, after], slot == CHUNKS // 2)
                project(gather_chunk(1, slot), [before, after], False)
        finish([before, after])
        return carry

    lax.fori_loop(1, half, gather_step, 0)
    kv_copy(block(1 - half)).start()
    kv_copy(block(half - 1)).start()
    last = block(half)
    prepare_turn([last])
    quiet = jnp.zeros((rows, cols), jnp.bfloat16)
    for i in range(CHUNKS):
        rs_in[(half if i < CHUNKS // 2 else 0) * CHUNKS + i] = quiet
    for slot in range(CHUNKS // 2):
        for way in range(2):
            i = gather_chunk(way, slot)
            gather_arrival(way, half, i).wait_recv()
            if slot < CHUNKS // 2 - 1:
                project(i, [last], slot == 0 and way == 0)
            else:
                project(i, [last], False, 0, 2)
    finish_pairs([last])
    kv_copy(last).start()
    for way in range(2):
        project(gather_chunk(way, CHUNKS // 2 - 1), [last], False, 2, 4)
    finish_queries([last])

    def attend(queries, pairs, row):
        keys = pairs[:, 0].reshape(tokens, head)
        values = pairs[:, 1].reshape(tokens, head)
        scores = lax.dot_general(
            queries, keys, (((1,), (1,)), ((), ())), preferred_element_type=jnp.float32
        )
        scores = scores * score_scale + bias[row : row + 1, :]
        raised = jnp.exp2(scores - jnp.max(scores, -1, keepdims=True))
        total = jnp.sum(raised, -1, keepdims=True)
        summed = jnp.dot(raised.astype(jnp.bfloat16), values, preferred_element_type=jnp.float32)
        return (summed / total).astype(jnp.bfloat16)

    def attend_self(blocks):
        picked = [q_all[b] for b in blocks]
        lhs = picked[0] if len(picked) == 1 else jnp.concatenate(picked, 0)
        both[: lhs.shape[0], :head] = attend(lhs, kv_own, 0)

    def attend_cross(blocks):
        picked = [c_all[b] for b in blocks]
        lhs = picked[0] if len(picked) == 1 else jnp.concatenate(picked, 0)
        both[: lhs.shape[0], head:] = attend(lhs, kv_far, 1)

    def expand(count, i):
        return jnp.dot(
            both[:count, :], w_out[:, i * cols : (i + 1) * cols], preferred_element_type=jnp.float32
        )

    def partial_piece(turn, blocks, piece):
        if piece == 0:
            attend_self(blocks)
        elif piece == 1:
            attend_cross(blocks)
        else:
            for i in range(2 * (piece - 2), 2 * (piece - 1)):
                term = expand(2 * rows, i)
                part[turn, 0, i] = term[:rows]
                part[turn, 1, i] = term[rows:]

    attend_self([last])
    for i in range(CHUNKS):
        part[0, 0, i] = jnp.dot(
            both[:rows, :head],
            w_out[:head, i * cols : (i + 1) * cols],
            preferred_element_type=jnp.float32,
        )
    pltpu.make_async_copy(kv_far, kv_far, kv_recv).wait()
    attend_cross([last])
    for i in (0, 2, 1, 3):
        way = 0 if i < CHUNKS // 2 else 1
        term = part[0, 0, i] + jnp.dot(
            both[:rows, head:],
            w_out[head:, i * cols : (i + 1) * cols],
            preferred_element_type=jnp.float32,
        )
        rs_out[way * half * CHUNKS + i] = term.astype(jnp.bfloat16)
        scatter_copy(way, 0, i).start()
    for piece in range(4):
        partial_piece(1, [block(half - 1), block(1 - half)], piece)

    def scatter_step(step, carry):
        turn = lax.rem(step, 2)
        following = [block(half - 1 - step), block(step + 1 - half)]
        for slot in range(CHUNKS):
            for way in range(2):
                i = scatter_chunk(way, slot)
                if slot >= CHUNKS // 2:
                    scatter_copy(way, step - 1, i).wait_recv()
                else:
                    pl.when(step > 1)(lambda way=way, i=i: scatter_copy(way, step - 1, i).wait_recv())
                running = rs_in[(way * half + step - 1) * CHUNKS + i].astype(jnp.float32) + part[turn, way, i]
                rs_out[(way * half + step) * CHUNKS + i] = running.astype(jnp.bfloat16)
                scatter_copy(way, step, i).start()
            partial_piece(1 - turn, following, slot)
        return carry

    lax.fori_loop(1, half, scatter_step, 0)
    for i in (0, 2, 1, 3):
        scatter_copy(0, half - 1, i).wait_recv()
        scatter_copy(1, half - 1, i).wait_recv()
        span = slice(i * cols, (i + 1) * cols)
        branch = part[half % 2, 0, i] + (
            rs_in[(half - 1) * CHUNKS + i].astype(jnp.float32)
            + rs_in[(2 * half - 1) * CHUNKS + i].astype(jnp.float32)
        )
        out_ref[:, span] = (
            h_ref[:, span].astype(jnp.float32) + mod_ref[2, :, span] * branch
        ).astype(jnp.bfloat16)

    moved = (2 * half - 1) * CHUNKS
    all_sent(rows_all, moved, out_sem.at[0]).wait_send()
    all_sent(kv_own, n, out_sem.at[1]).wait_send()
    all_sent(rs_out, moved, out_sem.at[2]).wait_send()


def local(n, hidden, modulation, qk_gains, counts, offsets, in_weights, out_weights):
    rows, width = hidden.shape[1:]
    head = in_weights.shape[-1]
    half = n // 2
    tokens = n * rows
    cols = width // CHUNKS
    frequency = np.repeat(
        np.exp(np.arange(head // 2, dtype=np.float64) * (-2.0 * math.log(rope_base) / head)), 2
    ).astype(np.float32)[None]
    vmem = pl.BlockSpec(memory_space=pltpu.VMEM)
    anywhere = pl.BlockSpec(memory_space=pl.ANY)
    updated = pl.pallas_call(
        functools.partial(kernel, n),
        out_shape=pltpu.VMEM((rows, width), jnp.bfloat16),
        in_specs=[anywhere] * 8,
        out_specs=vmem,
        scratch_shapes=[
            pltpu.VMEM((rows, width), jnp.bfloat16),
            pltpu.VMEM((3, 1, width), jnp.float32),
            pltpu.VMEM((3, 1, head), jnp.float32),
            pltpu.VMEM((1, head), jnp.float32),
            pltpu.SMEM((1, 2), jnp.int32),
            pltpu.SMEM((1, 2), jnp.int32),
            pltpu.VMEM((n * CHUNKS, rows, cols), jnp.bfloat16),
            pltpu.VMEM((width * 4, head), jnp.bfloat16),
            pltpu.VMEM((4 * 128, head), jnp.float32),
            pltpu.VMEM((width, 4 * head), jnp.bfloat16),
            pltpu.VMEM((2 * head, width), jnp.bfloat16),
            pltpu.VMEM((2 * rows, 4 * head), jnp.float32),
            pltpu.VMEM((n, rows, head), jnp.bfloat16),
            pltpu.VMEM((n, rows, head), jnp.bfloat16),
            pltpu.VMEM((n, 2, rows, head), jnp.bfloat16),
            pltpu.VMEM((n, 2, rows, head), jnp.bfloat16),
            pltpu.VMEM((2, tokens), jnp.float32),
            pltpu.VMEM((2, 2 * rows, head), jnp.float32),
            pltpu.VMEM((2 * rows, 2 * head), jnp.bfloat16),
            pltpu.VMEM((2, 2, CHUNKS, rows, cols), jnp.float32),
            pltpu.VMEM((2 * half * CHUNKS, rows, cols), jnp.bfloat16),
            pltpu.VMEM((2 * half * CHUNKS, rows, cols), jnp.bfloat16),
            pltpu.SemaphoreType.DMA((8,)),
            pltpu.SemaphoreType.DMA((3,)),
            pltpu.SemaphoreType.DMA((2, 4, CHUNKS)),
            pltpu.SemaphoreType.DMA,
        ],
        compiler_params=pltpu.CompilerParams(
            collective_id=0, has_side_effects=True, vmem_limit_bytes=56 * 1024 * 1024
        ),
    )(
        hidden[0],
        jnp.transpose(modulation, (1, 0, 2)),
        jnp.transpose(qk_gains, (1, 0, 2)),
        jnp.asarray(frequency),
        counts.T,
        offsets.T,
        in_weights.reshape(4 * width, head),
        out_weights.reshape(2 * head, width),
    )
    return updated[None]


def solution(mesh):
    return jax.shard_map(
        functools.partial(local, mesh.shape["tp"]),
        mesh=mesh,
        in_specs=(
            P("tower", ("grp", "tp"), None),
            P("tower", None, None),
            P("tower", None, "tp"),
            P(None, "grp"),
            P(None, "grp"),
            P("tower", None, None, "tp"),
            P("tower", None, "tp", None),
        ),
        out_specs=P("tower", ("grp", "tp"), None),
        check_vma=False,
    )
```

```python
import functools
import math

import jax
import jax.numpy as jnp
import numpy as np
from jax import lax
from jax.experimental import pallas as pl
from jax.experimental.pallas import tpu as pltpu
from jax.sharding import PartitionSpec as P

MESH = pl.DeviceIdType.MESH
epsilon = 1e-06
rope_base = 10000.0
masked_score = -1e30
CHUNKS = 4


def kernel(
    n,
    h_hbm,
    mod_hbm,
    gain_hbm,
    freq_hbm,
    cnt_hbm,
    off_hbm,
    win_hbm,
    wout_hbm,
    out_ref,
    h_ref,
    mod_ref,
    gain_ref,
    freq_ref,
    cnt_ref,
    off_ref,
    rows_all,
    raw,
    wide,
    w_in,
    w_out,
    acc,
    q_all,
    c_all,
    kv_own,
    kv_far,
    bias,
    trig,
    both,
    part,
    rs_in,
    rs_out,
    w_sem,
    out_sem,
    recv,
    kv_recv,
):
    half = n // 2
    me = lax.axis_index("tp")
    tower = lax.axis_index("tower")
    right = lax.rem(me + 1, n)
    left = lax.rem(me + n - 1, n)
    other = 1 - tower
    depth = recv.shape[1]
    rows, width = h_ref.shape
    head = gain_ref.shape[-1]
    cols = width // CHUNKS
    tokens = n * rows
    score_scale = math.log2(math.e) / math.sqrt(head)

    loads = [
        pltpu.make_async_copy(source, target, w_sem.at[j])
        for j, (source, target) in enumerate(
            (
                (h_hbm, h_ref),
                (mod_hbm, mod_ref),
                (win_hbm, raw),
                (cnt_hbm, cnt_ref),
                (off_hbm, off_ref),
                (gain_hbm, gain_ref),
                (freq_hbm, freq_ref),
                (wout_hbm, w_out),
            )
        )
    ]
    h_copy, mod_copy, win_copy, cnt_copy, off_copy, gain_copy, freq_copy, wout_copy = loads
    for load in loads:
        load.start()

    barrier = pltpu.get_barrier_semaphore()
    for where in ({"tp": left}, {"tp": right}, {"tower": other}):
        pl.semaphore_signal(barrier, inc=1, device_id=where, device_id_type=MESH)

    def block(offset):
        return lax.rem(me + offset + 2 * n, n)

    def gather_copy(way, step, i):
        piece = block(-step if way == 0 else step) * CHUNKS + i
        return pltpu.make_async_remote_copy(
            src_ref=rows_all.at[piece],
            dst_ref=rows_all.at[piece],
            send_sem=out_sem.at[0],
            recv_sem=recv.at[way, lax.rem(step, depth), i],
            device_id={"tp": right if way == 0 else left},
            device_id_type=MESH,
        )

    def gather_arrival(way, step, i):
        return gather_copy(way, step - 1, i)

    def place_of(b):
        return lax.rem(b - me + half - 1 + n, n)

    def kv_copy(b, recv_index=0):
        place = n - 1 if recv_index else place_of(b)
        return pltpu.make_async_remote_copy(
            src_ref=kv_own.at[place],
            dst_ref=kv_far.at[place],
            send_sem=out_sem.at[1],
            recv_sem=kv_recv.at[recv_index],
            device_id={"tower": other},
            device_id_type=MESH,
        )

    def scatter_copy(way, step, i):
        piece = (way * half + step) * CHUNKS + i
        return pltpu.make_async_remote_copy(
            src_ref=rs_out.at[piece],
            dst_ref=rs_in.at[piece],
            send_sem=out_sem.at[2],
            recv_sem=recv.at[way, lax.rem(step, depth), i],
            device_id={"tp": right if way == 0 else left},
            device_id_type=MESH,
        )

    def gather_chunk(way, slot):
        return slot if way == 0 else (slot + CHUNKS // 2) % CHUNKS

    def scatter_chunk(way, slot):
        return gather_chunk(1 - way, slot)

    def all_sent(ref, count, sem):
        return pltpu.make_async_remote_copy(
            src_ref=ref.at[pl.ds(0, count)],
            dst_ref=ref.at[pl.ds(0, count)],
            send_sem=sem,
            recv_sem=kv_recv.at[0],
            device_id={"tower": other},
            device_id_type=MESH,
        )

    h_copy.wait()
    mod_copy.wait()
    states = h_ref[...].astype(jnp.float32)
    centre = states - jnp.mean(states, -1, keepdims=True)
    spread = jnp.mean(centre * centre, -1, keepdims=True)
    normed = centre * lax.rsqrt(spread + epsilon) * (1.0 + mod_ref[1]) + mod_ref[0]
    normed = normed.astype(jnp.bfloat16)
    for i in range(CHUNKS):
        rows_all[me * CHUNKS + i] = normed[:, i * cols : (i + 1) * cols]

    pl.semaphore_wait(barrier, 3)
    for slot in range(CHUNKS):
        for way in range(2):
            gather_copy(way, 0, gather_chunk(way, slot)).start()

    cnt_copy.wait()
    key_index = lax.rem(
        lax.broadcasted_iota(jnp.int32, (1, tokens), 1) + (me + half + 1) * rows, tokens
    )
    bias[0:1, :] = jnp.where(key_index < cnt_ref[0, tower], 0.0, masked_score)
    bias[1:2, :] = jnp.where(key_index < cnt_ref[0, other], 0.0, masked_score)

    win_copy.wait()
    fold = wide.shape[0] // 4
    placed = (1, 2, 0, 3)

    def unfold(j, carry):
        wide[...] = raw[pl.ds(pl.multiple_of(j * 4 * fold, 4 * fold), 4 * fold), :].astype(jnp.float32)
        for place, c in enumerate(placed):
            w_in[pl.ds(pl.multiple_of(j * fold, fold), fold), place * head : (place + 1) * head] = wide[
                pl.ds(c, fold, stride=4), :
            ].astype(jnp.bfloat16)
        return carry

    lax.fori_loop(0, width // fold, unfold, 0)
    for load in (off_copy, gain_copy, freq_copy, wout_copy):
        load.wait()

    lane = lax.broadcasted_iota(jnp.int32, (1, head), 1)
    is_even = lax.rem(lane, 2) == 0
    offset = off_ref[0, tower]

    def row_positions(b):
        return offset + b * rows + lax.broadcasted_iota(jnp.int32, (rows, 1), 0)

    def project(i, blocks, first, begin=0, end=4):
        picked = [rows_all[b * CHUNKS + i] for b in blocks]
        lhs = picked[0] if len(picked) == 1 else jnp.concatenate(picked, 0)
        span = slice(begin * head, end * head)
        term = jnp.dot(lhs, w_in[i * cols : (i + 1) * cols, span], preferred_element_type=jnp.float32)
        if first:
            acc[: lhs.shape[0], span] = term
        else:
            acc[: lhs.shape[0], span] += term

    def prepare_turn(blocks):
        for j, b in enumerate(blocks):
            angles = row_positions(b).astype(jnp.float32) * freq_ref[...]
            sine = jnp.sin(angles)
            trig[0, j * rows : (j + 1) * rows] = jnp.cos(angles)
            trig[1, j * rows : (j + 1) * rows] = jnp.where(is_even, -sine, sine)

    def turned(count, place, g):
        x = acc[:count, place * head : (place + 1) * head]
        square = jnp.mean(x * x, -1, keepdims=True)
        x = x * lax.rsqrt(square + epsilon) * gain_ref[g]
        swapped = jnp.where(is_even, pltpu.roll(x, head - 1, 1), pltpu.roll(x, 1, 1))
        return (x * trig[0, :count] + swapped * trig[1, :count]).astype(jnp.bfloat16)

    def finish_pairs(blocks):
        count = len(blocks) * rows
        keys = turned(count, 0, 1)
        values = acc[:count, head : 2 * head].astype(jnp.bfloat16)
        for j, b in enumerate(blocks):
            span = slice(j * rows, (j + 1) * rows)
            kv_own[place_of(b), 0] = keys[span]
            kv_own[place_of(b), 1] = values[span]

    def finish_queries(blocks):
        count = len(blocks) * rows
        queries = turned(count, 2, 0)
        cross = turned(count, 3, 2)
        for j, b in enumerate(blocks):
            span = slice(j * rows, (j + 1) * rows)
            q_all[b] = queries[span]
            c_all[b] = cross[span]

    def finish(blocks):
        finish_pairs(blocks)
        finish_queries(blocks)

    for i in range(CHUNKS):
        project(i, [me], i == 0)
    prepare_turn([me])
    finish([me])

    def gather_step(step, carry):
        before, after = block(-step), block(step)
        prepare_turn([before, after])
        for slot in range(CHUNKS):
            for way in range(2):
                i = gather_chunk(way, slot)
                gather_arrival(way, step, i).wait_recv()
                if slot < CHUNKS // 2:
                    gather_copy(way, step, i).start()
                else:
                    pl.when(step < half - 1)(lambda way=way, i=i: gather_copy(way, step, i).start())
            if slot == 0:
                kv_copy(block(1 - step)).start()
                pl.when(step > 1)(lambda: kv_copy(block(step - 1)).start())
            if slot >= CHUNKS // 2:
                project(gather_chunk(0, slot), [before, after], slot == CHUNKS // 2)
                project(gather_chunk(1, slot), [before, after], False)
        finish([before, after])
        return carry

    lax.fori_loop(1, half, gather_step, 0)
    kv_copy(block(1 - half)).start()
    kv_copy(block(half - 1)).start()
    last = block(half)
    prepare_turn([last])
    quiet = jnp.zeros((rows, cols), jnp.bfloat16)
    for i in range(CHUNKS):
        rs_in[(half if i < CHUNKS // 2 else 0) * CHUNKS + i] = quiet
    for slot in range(CHUNKS // 2):
        for way in range(2):
            i = gather_chunk(way, slot)
            gather_arrival(way, half, i).wait_recv()
            if slot < CHUNKS // 2 - 1:
                project(i, [last], slot == 0 and way == 0)
            else:
                project(i, [last], False, 0, 2)
    finish_pairs([last])
    kv_copy(last, 1).start()
    for way in range(2):
        project(gather_chunk(way, CHUNKS // 2 - 1), [last], False, 2, 4)
    finish_queries([last])

    def attend(queries, pairs, row):
        keys = pairs[:, 0].reshape(tokens, head)
        values = pairs[:, 1].reshape(tokens, head)
        scores = lax.dot_general(
            queries, keys, (((1,), (1,)), ((), ())), preferred_element_type=jnp.float32
        )
        scores = scores * score_scale + bias[row : row + 1, :]
        raised = jnp.exp2(scores - jnp.max(scores, -1, keepdims=True))
        total = jnp.sum(raised, -1, keepdims=True)
        summed = jnp.dot(raised.astype(jnp.bfloat16), values, preferred_element_type=jnp.float32)
        return (summed / total).astype(jnp.bfloat16)

    def scored(queries, keys, row, begin, end):
        scores = lax.dot_general(
            queries,
            keys.reshape(end - begin, head),
            (((1,), (1,)), ((), ())),
            preferred_element_type=jnp.float32,
        )
        return scores * score_scale + bias[row : row + 1, begin:end]

    def attend_self(blocks):
        picked = [q_all[b] for b in blocks]
        lhs = picked[0] if len(picked) == 1 else jnp.concatenate(picked, 0)
        both[: lhs.shape[0], :head] = attend(lhs, kv_own, 0)

    def attend_cross(blocks):
        picked = [c_all[b] for b in blocks]
        lhs = picked[0] if len(picked) == 1 else jnp.concatenate(picked, 0)
        both[: lhs.shape[0], head:] = attend(lhs, kv_far, 1)

    def expand(count, i):
        return jnp.dot(
            both[:count, :], w_out[:, i * cols : (i + 1) * cols], preferred_element_type=jnp.float32
        )

    def partial_piece(turn, blocks, piece):
        if piece == 0:
            attend_self(blocks)
        elif piece == 1:
            attend_cross(blocks)
        else:
            for i in range(2 * (piece - 2), 2 * (piece - 1)):
                term = expand(2 * rows, i)
                part[turn, 0, i] = term[:rows]
                part[turn, 1, i] = term[rows:]

    pltpu.make_async_copy(
        kv_far.at[pl.ds(0, n - 1)], kv_far.at[pl.ds(0, n - 1)], kv_recv.at[0]
    ).wait()
    split = n - max(128 // rows, 1)
    cross = c_all[last]
    early = scored(cross, kv_far[:split, 0], 1, 0, split * rows)
    attend_self([last])
    early_max = jnp.max(early, -1, keepdims=True)
    early = jnp.exp2(early - early_max)
    early_total = jnp.sum(early, -1, keepdims=True)
    early_sum = jnp.dot(
        early.astype(jnp.bfloat16),
        kv_far[:split, 1].reshape(split * rows, head),
        preferred_element_type=jnp.float32,
    )
    for i in range(CHUNKS):
        part[0, 0, i] = jnp.dot(
            both[:rows, :head],
            w_out[:head, i * cols : (i + 1) * cols],
            preferred_element_type=jnp.float32,
        )
    kv_copy(last, 1).wait_recv()
    late = scored(cross, kv_far[split:, 0], 1, split * rows, tokens)
    top = jnp.maximum(early_max, jnp.max(late, -1, keepdims=True))
    late = jnp.exp2(late - top)
    kept = jnp.exp2(early_max - top)
    total = kept * early_total + jnp.sum(late, -1, keepdims=True)
    summed = kept * early_sum + jnp.dot(
        late.astype(jnp.bfloat16),
        kv_far[split:, 1].reshape(tokens - split * rows, head),
        preferred_element_type=jnp.float32,
    )
    both[:rows, head:] = (summed / total).astype(jnp.bfloat16)
    for i in (0, 2, 1, 3):
        way = 0 if i < CHUNKS // 2 else 1
        term = part[0, 0, i] + jnp.dot(
            both[:rows, head:],
            w_out[head:, i * cols : (i + 1) * cols],
            preferred_element_type=jnp.float32,
        )
        rs_out[way * half * CHUNKS + i] = term.astype(jnp.bfloat16)
        scatter_copy(way, 0, i).start()
    for piece in range(4):
        partial_piece(1, [block(half - 1), block(1 - half)], piece)

    def scatter_step(step, carry):
        turn = lax.rem(step, 2)
        following = [block(half - 1 - step), block(step + 1 - half)]
        for slot in range(CHUNKS):
            for way in range(2):
                i = scatter_chunk(way, slot)
                if slot >= CHUNKS // 2:
                    scatter_copy(way, step - 1, i).wait_recv()
                else:
                    pl.when(step > 1)(lambda way=way, i=i: scatter_copy(way, step - 1, i).wait_recv())
                running = rs_in[(way * half + step - 1) * CHUNKS + i].astype(jnp.float32) + part[turn, way, i]
                rs_out[(way * half + step) * CHUNKS + i] = running.astype(jnp.bfloat16)
                scatter_copy(way, step, i).start()
            partial_piece(1 - turn, following, slot)
        return carry

    lax.fori_loop(1, half, scatter_step, 0)
    for i in (0, 2, 1, 3):
        scatter_copy(0, half - 1, i).wait_recv()
        scatter_copy(1, half - 1, i).wait_recv()
        span = slice(i * cols, (i + 1) * cols)
        branch = part[half % 2, 0, i] + (
            rs_in[(half - 1) * CHUNKS + i].astype(jnp.float32)
            + rs_in[(2 * half - 1) * CHUNKS + i].astype(jnp.float32)
        )
        out_ref[:, span] = (
            h_ref[:, span].astype(jnp.float32) + mod_ref[2, :, span] * branch
        ).astype(jnp.bfloat16)

    moved = (2 * half - 1) * CHUNKS
    all_sent(rows_all, moved, out_sem.at[0]).wait_send()
    all_sent(kv_own, n, out_sem.at[1]).wait_send()
    all_sent(rs_out, moved, out_sem.at[2]).wait_send()


def local(n, hidden, modulation, qk_gains, counts, offsets, in_weights, out_weights):
    rows, width = hidden.shape[1:]
    head = in_weights.shape[-1]
    half = n // 2
    tokens = n * rows
    cols = width // CHUNKS
    frequency = np.repeat(
        np.exp(np.arange(head // 2, dtype=np.float64) * (-2.0 * math.log(rope_base) / head)), 2
    ).astype(np.float32)[None]
    vmem = pl.BlockSpec(memory_space=pltpu.VMEM)
    anywhere = pl.BlockSpec(memory_space=pl.ANY)
    updated = pl.pallas_call(
        functools.partial(kernel, n),
        out_shape=pltpu.VMEM((rows, width), jnp.bfloat16),
        in_specs=[anywhere] * 8,
        out_specs=vmem,
        scratch_shapes=[
            pltpu.VMEM((rows, width), jnp.bfloat16),
            pltpu.VMEM((3, 1, width), jnp.float32),
            pltpu.VMEM((3, 1, head), jnp.float32),
            pltpu.VMEM((1, head), jnp.float32),
            pltpu.SMEM((1, 2), jnp.int32),
            pltpu.SMEM((1, 2), jnp.int32),
            pltpu.VMEM((n * CHUNKS, rows, cols), jnp.bfloat16),
            pltpu.VMEM((width * 4, head), jnp.bfloat16),
            pltpu.VMEM((4 * 128, head), jnp.float32),
            pltpu.VMEM((width, 4 * head), jnp.bfloat16),
            pltpu.VMEM((2 * head, width), jnp.bfloat16),
            pltpu.VMEM((2 * rows, 4 * head), jnp.float32),
            pltpu.VMEM((n, rows, head), jnp.bfloat16),
            pltpu.VMEM((n, rows, head), jnp.bfloat16),
            pltpu.VMEM((n, 2, rows, head), jnp.bfloat16),
            pltpu.VMEM((n, 2, rows, head), jnp.bfloat16),
            pltpu.VMEM((2, tokens), jnp.float32),
            pltpu.VMEM((2, 2 * rows, head), jnp.float32),
            pltpu.VMEM((2 * rows, 2 * head), jnp.bfloat16),
            pltpu.VMEM((2, 2, CHUNKS, rows, cols), jnp.float32),
            pltpu.VMEM((2 * half * CHUNKS, rows, cols), jnp.bfloat16),
            pltpu.VMEM((2 * half * CHUNKS, rows, cols), jnp.bfloat16),
            pltpu.SemaphoreType.DMA((8,)),
            pltpu.SemaphoreType.DMA((3,)),
            pltpu.SemaphoreType.DMA((2, 4, CHUNKS)),
            pltpu.SemaphoreType.DMA((2,)),
        ],
        compiler_params=pltpu.CompilerParams(
            collective_id=0, has_side_effects=True, vmem_limit_bytes=56 * 1024 * 1024
        ),
    )(
        hidden[0],
        jnp.transpose(modulation, (1, 0, 2)),
        jnp.transpose(qk_gains, (1, 0, 2)),
        jnp.asarray(frequency),
        counts.T,
        offsets.T,
        in_weights.reshape(4 * width, head),
        out_weights.reshape(2 * head, width),
    )
    return updated[None]


def solution(mesh):
    return jax.shard_map(
        functools.partial(local, mesh.shape["tp"]),
        mesh=mesh,
        in_specs=(
            P("tower", ("grp", "tp"), None),
            P("tower", None, None),
            P("tower", None, "tp"),
            P(None, "grp"),
            P(None, "grp"),
            P("tower", None, None, "tp"),
            P("tower", None, "tp", None),
        ),
        out_specs=P("tower", ("grp", "tp"), None),
        check_vma=False,
    )
```

```python
import functools
import math

import jax
import jax.numpy as jnp
import numpy as np
from jax import lax
from jax.experimental import pallas as pl
from jax.experimental.pallas import tpu as pltpu
from jax.sharding import PartitionSpec as P

MESH = pl.DeviceIdType.MESH
epsilon = 1e-06
rope_base = 10000.0
masked_score = -1e30
CHUNKS = 4


def kernel(
    n,
    h_hbm,
    mod_hbm,
    gain_hbm,
    freq_hbm,
    cnt_hbm,
    off_hbm,
    win_hbm,
    wout_hbm,
    out_ref,
    h_ref,
    mod_ref,
    gain_ref,
    freq_ref,
    cnt_ref,
    off_ref,
    rows_all,
    raw,
    wide,
    w_in,
    w_out,
    acc,
    q_all,
    c_all,
    kv_own,
    kv_far,
    bias,
    trig,
    both,
    part,
    rs_in,
    rs_out,
    w_sem,
    out_sem,
    recv,
    kv_recv,
):
    half = n // 2
    me = lax.axis_index("tp")
    tower = lax.axis_index("tower")
    right = lax.rem(me + 1, n)
    left = lax.rem(me + n - 1, n)
    other = 1 - tower
    depth = recv.shape[1]
    rows, width = h_ref.shape
    head = gain_ref.shape[-1]
    cols = width // CHUNKS
    tokens = n * rows
    score_scale = math.log2(math.e) / math.sqrt(head)

    barrier = pltpu.get_barrier_semaphore()
    for where in ({"tp": left}, {"tp": right}, {"tower": other}):
        pl.semaphore_signal(barrier, inc=1, device_id=where, device_id_type=MESH)

    loads = [
        pltpu.make_async_copy(source, target, w_sem.at[j])
        for j, (source, target) in enumerate(
            (
                (h_hbm, h_ref),
                (mod_hbm, mod_ref),
                (win_hbm, raw),
                (cnt_hbm, cnt_ref),
                (off_hbm, off_ref),
                (gain_hbm, gain_ref),
                (freq_hbm, freq_ref),
                (wout_hbm, w_out),
            )
        )
    ]
    h_copy, mod_copy, win_copy, cnt_copy, off_copy, gain_copy, freq_copy, wout_copy = loads
    for load in loads:
        load.start()

    def block(offset):
        return lax.rem(me + offset + 2 * n, n)

    def gather_copy(way, step, i):
        piece = block(-step if way == 0 else step) * CHUNKS + i
        return pltpu.make_async_remote_copy(
            src_ref=rows_all.at[piece],
            dst_ref=rows_all.at[piece],
            send_sem=out_sem.at[0],
            recv_sem=recv.at[way, lax.rem(step, depth), i],
            device_id={"tp": right if way == 0 else left},
            device_id_type=MESH,
        )

    def gather_arrival(way, step, i):
        return gather_copy(way, step - 1, i)

    def place_of(b):
        return lax.rem(b - me + half - 1 + n, n)

    def kv_copy(b, recv_index=0):
        place = n - 1 if recv_index else place_of(b)
        return pltpu.make_async_remote_copy(
            src_ref=kv_own.at[place],
            dst_ref=kv_far.at[place],
            send_sem=out_sem.at[1],
            recv_sem=kv_recv.at[recv_index],
            device_id={"tower": other},
            device_id_type=MESH,
        )

    def scatter_copy(way, step, i):
        piece = (way * half + step) * CHUNKS + i
        return pltpu.make_async_remote_copy(
            src_ref=rs_out.at[piece],
            dst_ref=rs_in.at[piece],
            send_sem=out_sem.at[2],
            recv_sem=recv.at[way, lax.rem(step, depth), i],
            device_id={"tp": right if way == 0 else left},
            device_id_type=MESH,
        )

    def gather_chunk(way, slot):
        return slot if way == 0 else (slot + CHUNKS // 2) % CHUNKS

    def scatter_chunk(way, slot):
        return gather_chunk(1 - way, slot)

    def all_sent(ref, count, sem):
        return pltpu.make_async_remote_copy(
            src_ref=ref.at[pl.ds(0, count)],
            dst_ref=ref.at[pl.ds(0, count)],
            send_sem=sem,
            recv_sem=kv_recv.at[0],
            device_id={"tower": other},
            device_id_type=MESH,
        )

    h_copy.wait()
    mod_copy.wait()
    states = h_ref[...].astype(jnp.float32)
    centre = states - jnp.mean(states, -1, keepdims=True)
    spread = jnp.mean(centre * centre, -1, keepdims=True)
    inverse = lax.rsqrt(spread + epsilon)

    def normalize(i):
        span = slice(i * cols, (i + 1) * cols)
        normed = centre[:, span] * inverse * (1.0 + mod_ref[1, :, span]) + mod_ref[0, :, span]
        rows_all[me * CHUNKS + i] = normed.astype(jnp.bfloat16)

    for way in range(2):
        normalize(gather_chunk(way, 0))
    pl.semaphore_wait(barrier, 3)
    for slot in range(CHUNKS):
        for way in range(2):
            gather_copy(way, 0, gather_chunk(way, slot)).start()
            if slot + 1 < CHUNKS // 2:
                normalize(gather_chunk(way, slot + 1))

    cnt_copy.wait()
    key_index = lax.rem(
        lax.broadcasted_iota(jnp.int32, (1, tokens), 1) + (me + half + 1) * rows, tokens
    )
    bias[0:1, :] = jnp.where(key_index < cnt_ref[0, tower], 0.0, masked_score)
    bias[1:2, :] = jnp.where(key_index < cnt_ref[0, other], 0.0, masked_score)

    win_copy.wait()
    fold = wide.shape[0] // 4
    placed = (1, 2, 0, 3)

    def unfold(j, carry):
        wide[...] = raw[pl.ds(pl.multiple_of(j * 4 * fold, 4 * fold), 4 * fold), :].astype(jnp.float32)
        for place, c in enumerate(placed):
            w_in[pl.ds(pl.multiple_of(j * fold, fold), fold), place * head : (place + 1) * head] = wide[
                pl.ds(c, fold, stride=4), :
            ].astype(jnp.bfloat16)
        return carry

    lax.fori_loop(0, width // fold, unfold, 0)
    for load in (off_copy, gain_copy, freq_copy, wout_copy):
        load.wait()

    lane = lax.broadcasted_iota(jnp.int32, (1, head), 1)
    is_even = lax.rem(lane, 2) == 0
    offset = off_ref[0, tower]

    def row_positions(b):
        return offset + b * rows + lax.broadcasted_iota(jnp.int32, (rows, 1), 0)

    def project(i, blocks, first, begin=0, end=4):
        picked = [rows_all[b * CHUNKS + i] for b in blocks]
        lhs = picked[0] if len(picked) == 1 else jnp.concatenate(picked, 0)
        span = slice(begin * head, end * head)
        term = jnp.dot(lhs, w_in[i * cols : (i + 1) * cols, span], preferred_element_type=jnp.float32)
        if first:
            acc[: lhs.shape[0], span] = term
        else:
            acc[: lhs.shape[0], span] += term

    def prepare_turn(blocks):
        for j, b in enumerate(blocks):
            angles = row_positions(b).astype(jnp.float32) * freq_ref[...]
            sine = jnp.sin(angles)
            trig[0, j * rows : (j + 1) * rows] = jnp.cos(angles)
            trig[1, j * rows : (j + 1) * rows] = jnp.where(is_even, -sine, sine)

    def turned(count, place, g):
        x = acc[:count, place * head : (place + 1) * head]
        square = jnp.mean(x * x, -1, keepdims=True)
        x = x * lax.rsqrt(square + epsilon) * gain_ref[g]
        swapped = jnp.where(is_even, pltpu.roll(x, head - 1, 1), pltpu.roll(x, 1, 1))
        return (x * trig[0, :count] + swapped * trig[1, :count]).astype(jnp.bfloat16)

    def finish_pairs(blocks):
        count = len(blocks) * rows
        keys = turned(count, 0, 1)
        values = acc[:count, head : 2 * head].astype(jnp.bfloat16)
        for j, b in enumerate(blocks):
            span = slice(j * rows, (j + 1) * rows)
            kv_own[place_of(b), 0] = keys[span]
            kv_own[place_of(b), 1] = values[span]

    def finish_queries(blocks):
        count = len(blocks) * rows
        queries = turned(count, 2, 0)
        cross = turned(count, 3, 2)
        for j, b in enumerate(blocks):
            span = slice(j * rows, (j + 1) * rows)
            q_all[b] = queries[span]
            c_all[b] = cross[span]

    def finish(blocks):
        finish_pairs(blocks)
        finish_queries(blocks)

    for i in range(CHUNKS):
        project(i, [me], i == 0)
    prepare_turn([me])
    finish([me])

    def gather_step(step, carry):
        before, after = block(-step), block(step)
        prepare_turn([before, after])
        for slot in range(CHUNKS):
            for way in range(2):
                i = gather_chunk(way, slot)
                gather_arrival(way, step, i).wait_recv()
                if slot < CHUNKS // 2:
                    gather_copy(way, step, i).start()
                else:
                    pl.when(step < half - 1)(lambda way=way, i=i: gather_copy(way, step, i).start())
            if slot == 0:
                kv_copy(block(1 - step)).start()
                pl.when(step > 1)(lambda: kv_copy(block(step - 1)).start())
            if slot >= CHUNKS // 2:
                project(gather_chunk(0, slot), [before, after], slot == CHUNKS // 2)
                project(gather_chunk(1, slot), [before, after], False)
        finish([before, after])
        return carry

    lax.fori_loop(1, half, gather_step, 0)
    kv_copy(block(1 - half)).start()
    kv_copy(block(half - 1)).start()
    last = block(half)
    prepare_turn([last])
    quiet = jnp.zeros((rows, cols), jnp.bfloat16)
    for i in range(CHUNKS):
        rs_in[(half if i < CHUNKS // 2 else 0) * CHUNKS + i] = quiet
    for slot in range(CHUNKS // 2):
        for way in range(2):
            i = gather_chunk(way, slot)
            gather_arrival(way, half, i).wait_recv()
            if slot < CHUNKS // 2 - 1:
                project(i, [last], slot == 0 and way == 0)
            else:
                project(i, [last], False, 0, 2)
    finish_pairs([last])
    kv_copy(last, 1).start()
    for way in range(2):
        project(gather_chunk(way, CHUNKS // 2 - 1), [last], False, 2, 4)
    finish_queries([last])

    def attend(queries, pairs, row):
        keys = pairs[:, 0].reshape(tokens, head)
        values = pairs[:, 1].reshape(tokens, head)
        scores = lax.dot_general(
            queries, keys, (((1,), (1,)), ((), ())), preferred_element_type=jnp.float32
        )
        scores = scores * score_scale + bias[row : row + 1, :]
        raised = jnp.exp2(scores - jnp.max(scores, -1, keepdims=True))
        total = jnp.sum(raised, -1, keepdims=True)
        summed = jnp.dot(raised.astype(jnp.bfloat16), values, preferred_element_type=jnp.float32)
        return (summed / total).astype(jnp.bfloat16)

    def scored(queries, keys, row, begin, end):
        scores = lax.dot_general(
            queries,
            keys.reshape(end - begin, head),
            (((1,), (1,)), ((), ())),
            preferred_element_type=jnp.float32,
        )
        return scores * score_scale + bias[row : row + 1, begin:end]

    def attend_self(blocks):
        picked = [q_all[b] for b in blocks]
        lhs = picked[0] if len(picked) == 1 else jnp.concatenate(picked, 0)
        both[: lhs.shape[0], :head] = attend(lhs, kv_own, 0)

    def attend_cross(blocks):
        picked = [c_all[b] for b in blocks]
        lhs = picked[0] if len(picked) == 1 else jnp.concatenate(picked, 0)
        both[: lhs.shape[0], head:] = attend(lhs, kv_far, 1)

    def expand(count, i):
        return jnp.dot(
            both[:count, :], w_out[:, i * cols : (i + 1) * cols], preferred_element_type=jnp.float32
        )

    def partial_piece(turn, blocks, piece):
        if piece == 0:
            attend_self(blocks)
        elif piece == 1:
            attend_cross(blocks)
        else:
            for i in range(2 * (piece - 2), 2 * (piece - 1)):
                term = expand(2 * rows, i)
                part[turn, 0, i] = term[:rows]
                part[turn, 1, i] = term[rows:]

    pltpu.make_async_copy(
        kv_far.at[pl.ds(0, n - 1)], kv_far.at[pl.ds(0, n - 1)], kv_recv.at[0]
    ).wait()
    split = n - max(128 // rows, 1)
    cross = c_all[last]
    early = scored(cross, kv_far[:split, 0], 1, 0, split * rows)
    attend_self([last])
    early_max = jnp.max(early, -1, keepdims=True)
    early = jnp.exp2(early - early_max)
    early_total = jnp.sum(early, -1, keepdims=True)
    early_sum = jnp.dot(
        early.astype(jnp.bfloat16),
        kv_far[:split, 1].reshape(split * rows, head),
        preferred_element_type=jnp.float32,
    )
    for i in range(CHUNKS):
        part[0, 0, i] = jnp.dot(
            both[:rows, :head],
            w_out[:head, i * cols : (i + 1) * cols],
            preferred_element_type=jnp.float32,
        )
    kv_copy(last, 1).wait_recv()
    late = scored(cross, kv_far[split:, 0], 1, split * rows, tokens)
    top = jnp.maximum(early_max, jnp.max(late, -1, keepdims=True))
    late = jnp.exp2(late - top)
    kept = jnp.exp2(early_max - top)
    total = kept * early_total + jnp.sum(late, -1, keepdims=True)
    summed = kept * early_sum + jnp.dot(
        late.astype(jnp.bfloat16),
        kv_far[split:, 1].reshape(tokens - split * rows, head),
        preferred_element_type=jnp.float32,
    )
    both[:rows, head:] = (summed / total).astype(jnp.bfloat16)
    for i in (0, 2, 1, 3):
        way = 0 if i < CHUNKS // 2 else 1
        term = part[0, 0, i] + jnp.dot(
            both[:rows, head:],
            w_out[head:, i * cols : (i + 1) * cols],
            preferred_element_type=jnp.float32,
        )
        rs_out[way * half * CHUNKS + i] = term.astype(jnp.bfloat16)
        scatter_copy(way, 0, i).start()
    for piece in range(4):
        partial_piece(1, [block(half - 1), block(1 - half)], piece)

    def scatter_step(step, carry):
        turn = lax.rem(step, 2)
        following = [block(half - 1 - step), block(step + 1 - half)]
        for slot in range(CHUNKS):
            for way in range(2):
                i = scatter_chunk(way, slot)
                if slot >= CHUNKS // 2:
                    scatter_copy(way, step - 1, i).wait_recv()
                else:
                    pl.when(step > 1)(lambda way=way, i=i: scatter_copy(way, step - 1, i).wait_recv())
                running = rs_in[(way * half + step - 1) * CHUNKS + i].astype(jnp.float32) + part[turn, way, i]
                rs_out[(way * half + step) * CHUNKS + i] = running.astype(jnp.bfloat16)
                scatter_copy(way, step, i).start()
            partial_piece(1 - turn, following, slot)
        return carry

    lax.fori_loop(1, half, scatter_step, 0)
    for i in (0, 2, 1, 3):
        scatter_copy(0, half - 1, i).wait_recv()
        scatter_copy(1, half - 1, i).wait_recv()
        span = slice(i * cols, (i + 1) * cols)
        branch = part[half % 2, 0, i] + (
            rs_in[(half - 1) * CHUNKS + i].astype(jnp.float32)
            + rs_in[(2 * half - 1) * CHUNKS + i].astype(jnp.float32)
        )
        out_ref[:, span] = (
            h_ref[:, span].astype(jnp.float32) + mod_ref[2, :, span] * branch
        ).astype(jnp.bfloat16)

    moved = (2 * half - 1) * CHUNKS
    all_sent(rows_all, moved, out_sem.at[0]).wait_send()
    all_sent(kv_own, n, out_sem.at[1]).wait_send()
    all_sent(rs_out, moved, out_sem.at[2]).wait_send()


def local(n, hidden, modulation, qk_gains, counts, offsets, in_weights, out_weights):
    rows, width = hidden.shape[1:]
    head = in_weights.shape[-1]
    half = n // 2
    tokens = n * rows
    cols = width // CHUNKS
    frequency = np.repeat(
        np.exp(np.arange(head // 2, dtype=np.float64) * (-2.0 * math.log(rope_base) / head)), 2
    ).astype(np.float32)[None]
    vmem = pl.BlockSpec(memory_space=pltpu.VMEM)
    anywhere = pl.BlockSpec(memory_space=pl.ANY)
    updated = pl.pallas_call(
        functools.partial(kernel, n),
        out_shape=pltpu.VMEM((rows, width), jnp.bfloat16),
        in_specs=[anywhere] * 8,
        out_specs=vmem,
        scratch_shapes=[
            pltpu.VMEM((rows, width), jnp.bfloat16),
            pltpu.VMEM((3, 1, width), jnp.float32),
            pltpu.VMEM((3, 1, head), jnp.float32),
            pltpu.VMEM((1, head), jnp.float32),
            pltpu.SMEM((1, 2), jnp.int32),
            pltpu.SMEM((1, 2), jnp.int32),
            pltpu.VMEM((n * CHUNKS, rows, cols), jnp.bfloat16),
            pltpu.VMEM((width * 4, head), jnp.bfloat16),
            pltpu.VMEM((4 * 128, head), jnp.float32),
            pltpu.VMEM((width, 4 * head), jnp.bfloat16),
            pltpu.VMEM((2 * head, width), jnp.bfloat16),
            pltpu.VMEM((2 * rows, 4 * head), jnp.float32),
            pltpu.VMEM((n, rows, head), jnp.bfloat16),
            pltpu.VMEM((n, rows, head), jnp.bfloat16),
            pltpu.VMEM((n, 2, rows, head), jnp.bfloat16),
            pltpu.VMEM((n, 2, rows, head), jnp.bfloat16),
            pltpu.VMEM((2, tokens), jnp.float32),
            pltpu.VMEM((2, 2 * rows, head), jnp.float32),
            pltpu.VMEM((2 * rows, 2 * head), jnp.bfloat16),
            pltpu.VMEM((2, 2, CHUNKS, rows, cols), jnp.float32),
            pltpu.VMEM((2 * half * CHUNKS, rows, cols), jnp.bfloat16),
            pltpu.VMEM((2 * half * CHUNKS, rows, cols), jnp.bfloat16),
            pltpu.SemaphoreType.DMA((8,)),
            pltpu.SemaphoreType.DMA((3,)),
            pltpu.SemaphoreType.DMA((2, 4, CHUNKS)),
            pltpu.SemaphoreType.DMA((2,)),
        ],
        compiler_params=pltpu.CompilerParams(
            collective_id=0, has_side_effects=True, vmem_limit_bytes=56 * 1024 * 1024
        ),
    )(
        hidden[0],
        jnp.transpose(modulation, (1, 0, 2)),
        jnp.transpose(qk_gains, (1, 0, 2)),
        jnp.asarray(frequency),
        counts.T,
        offsets.T,
        in_weights.reshape(4 * width, head),
        out_weights.reshape(2 * head, width),
    )
    return updated[None]


def solution(mesh):
    return jax.shard_map(
        functools.partial(local, mesh.shape["tp"]),
        mesh=mesh,
        in_specs=(
            P("tower", ("grp", "tp"), None),
            P("tower", None, None),
            P("tower", None, "tp"),
            P(None, "grp"),
            P(None, "grp"),
            P("tower", None, None, "tp"),
            P("tower", None, "tp", None),
        ),
        out_specs=P("tower", ("grp", "tp"), None),
        check_vma=False,
    )
```

```python
import functools
import math

import jax
import jax.numpy as jnp
import numpy as np
from jax import lax
from jax.experimental import pallas as pl
from jax.experimental.pallas import tpu as pltpu
from jax.sharding import PartitionSpec as P

MESH = pl.DeviceIdType.MESH
epsilon = 1e-06
rope_base = 10000.0
masked_score = -1e30
CHUNKS = 4


def kernel(
    n,
    h_hbm,
    mod_hbm,
    gain_hbm,
    freq_hbm,
    cnt_hbm,
    off_hbm,
    win_hbm,
    wout_hbm,
    out_ref,
    h_ref,
    mod_ref,
    gain_ref,
    freq_ref,
    cnt_ref,
    off_ref,
    rows_all,
    raw,
    wide,
    w_in,
    w_out,
    acc,
    q_all,
    c_all,
    kv_own,
    kv_far,
    bias,
    trig,
    both,
    part,
    rs_in,
    rs_out,
    w_sem,
    out_sem,
    recv,
    kv_recv,
):
    half = n // 2
    me = lax.axis_index("tp")
    tower = lax.axis_index("tower")
    right = lax.rem(me + 1, n)
    left = lax.rem(me + n - 1, n)
    other = 1 - tower
    depth = recv.shape[1]
    rows, width = h_ref.shape
    head = gain_ref.shape[-1]
    cols = width // CHUNKS
    tokens = n * rows
    score_scale = math.log2(math.e) / math.sqrt(head)

    barrier = pltpu.get_barrier_semaphore()
    for where in ({"tp": left}, {"tp": right}, {"tower": other}):
        pl.semaphore_signal(barrier, inc=1, device_id=where, device_id_type=MESH)

    loads = [
        pltpu.make_async_copy(source, target, w_sem.at[j])
        for j, (source, target) in enumerate(
            (
                (h_hbm, h_ref),
                (mod_hbm, mod_ref),
                (win_hbm, raw),
                (cnt_hbm, cnt_ref),
                (off_hbm, off_ref),
                (gain_hbm, gain_ref),
                (freq_hbm, freq_ref),
                (wout_hbm, w_out),
            )
        )
    ]
    h_copy, mod_copy, win_copy, cnt_copy, off_copy, gain_copy, freq_copy, wout_copy = loads
    for load in loads:
        load.start()

    def block(offset):
        return lax.rem(me + offset + 2 * n, n)

    def gather_copy(way, step, i):
        piece = block(-step if way == 0 else step) * CHUNKS + i
        return pltpu.make_async_remote_copy(
            src_ref=rows_all.at[piece],
            dst_ref=rows_all.at[piece],
            send_sem=out_sem.at[0],
            recv_sem=recv.at[way, lax.rem(step, depth), i],
            device_id={"tp": right if way == 0 else left},
            device_id_type=MESH,
        )

    def gather_arrival(way, step, i):
        return gather_copy(way, step - 1, i)

    def place_of(b):
        return lax.rem(b - me + half - 1 + n, n)

    def kv_copy(b, recv_index=0):
        place = n - 1 if recv_index else place_of(b)
        return pltpu.make_async_remote_copy(
            src_ref=kv_own.at[place],
            dst_ref=kv_far.at[place],
            send_sem=out_sem.at[1],
            recv_sem=kv_recv.at[recv_index],
            device_id={"tower": other},
            device_id_type=MESH,
        )

    def scatter_copy(way, step, i):
        piece = (way * half + step) * CHUNKS + i
        return pltpu.make_async_remote_copy(
            src_ref=rs_out.at[piece],
            dst_ref=rs_in.at[piece],
            send_sem=out_sem.at[2],
            recv_sem=recv.at[way, lax.rem(step, depth), i],
            device_id={"tp": right if way == 0 else left},
            device_id_type=MESH,
        )

    def gather_chunk(way, slot):
        return slot if way == 0 else (slot + CHUNKS // 2) % CHUNKS

    def scatter_chunk(way, slot):
        return gather_chunk(1 - way, slot)

    def all_sent(ref, count, sem):
        return pltpu.make_async_remote_copy(
            src_ref=ref.at[pl.ds(0, count)],
            dst_ref=ref.at[pl.ds(0, count)],
            send_sem=sem,
            recv_sem=kv_recv.at[0],
            device_id={"tower": other},
            device_id_type=MESH,
        )

    h_copy.wait()
    mod_copy.wait()
    states = h_ref[...].astype(jnp.float32)
    centre = states - jnp.mean(states, -1, keepdims=True)
    spread = jnp.mean(centre * centre, -1, keepdims=True)
    inverse = lax.rsqrt(spread + epsilon)

    def normalize(i):
        span = slice(i * cols, (i + 1) * cols)
        normed = centre[:, span] * inverse * (1.0 + mod_ref[1, :, span]) + mod_ref[0, :, span]
        rows_all[me * CHUNKS + i] = normed.astype(jnp.bfloat16)

    for way in range(2):
        normalize(gather_chunk(way, 0))
    pl.semaphore_wait(barrier, 3)
    for slot in range(CHUNKS):
        for way in range(2):
            gather_copy(way, 0, gather_chunk(way, slot)).start()
            if slot + 1 < CHUNKS // 2:
                normalize(gather_chunk(way, slot + 1))

    cnt_copy.wait()
    key_index = lax.rem(
        lax.broadcasted_iota(jnp.int32, (1, tokens), 1) + (me + half + 1) * rows, tokens
    )
    bias[0:1, :] = jnp.where(key_index < cnt_ref[0, tower], 0.0, masked_score)
    bias[1:2, :] = jnp.where(key_index < cnt_ref[0, other], 0.0, masked_score)

    win_copy.wait()
    fold = wide.shape[0] // 4
    placed = (1, 2, 0, 3)

    def unfold(j, carry):
        wide[...] = raw[pl.ds(pl.multiple_of(j * 4 * fold, 4 * fold), 4 * fold), :].astype(jnp.float32)
        for place, c in enumerate(placed):
            w_in[pl.ds(pl.multiple_of(j * fold, fold), fold), place * head : (place + 1) * head] = wide[
                pl.ds(c, fold, stride=4), :
            ].astype(jnp.bfloat16)
        return carry

    lax.fori_loop(0, width // fold, unfold, 0)
    for load in (off_copy, gain_copy, freq_copy, wout_copy):
        load.wait()

    lane = lax.broadcasted_iota(jnp.int32, (1, head), 1)
    is_even = lax.rem(lane, 2) == 0
    offset = off_ref[0, tower]

    def row_positions(b):
        return offset + b * rows + lax.broadcasted_iota(jnp.int32, (rows, 1), 0)

    def project(i, blocks, first, begin=0, end=4):
        picked = [rows_all[b * CHUNKS + i] for b in blocks]
        lhs = picked[0] if len(picked) == 1 else jnp.concatenate(picked, 0)
        span = slice(begin * head, end * head)
        term = jnp.dot(lhs, w_in[i * cols : (i + 1) * cols, span], preferred_element_type=jnp.float32)
        if first:
            acc[: lhs.shape[0], span] = term
        else:
            acc[: lhs.shape[0], span] += term

    def prepare_turn(blocks):
        for j, b in enumerate(blocks):
            angles = row_positions(b).astype(jnp.float32) * freq_ref[...]
            sine = jnp.sin(angles)
            trig[0, j * rows : (j + 1) * rows] = jnp.cos(angles)
            trig[1, j * rows : (j + 1) * rows] = jnp.where(is_even, -sine, sine)

    def turned(count, place, g):
        x = acc[:count, place * head : (place + 1) * head]
        square = jnp.mean(x * x, -1, keepdims=True)
        x = x * lax.rsqrt(square + epsilon) * gain_ref[g]
        swapped = jnp.where(is_even, pltpu.roll(x, head - 1, 1), pltpu.roll(x, 1, 1))
        return (x * trig[0, :count] + swapped * trig[1, :count]).astype(jnp.bfloat16)

    def finish_pairs(blocks):
        count = len(blocks) * rows
        keys = turned(count, 0, 1)
        values = acc[:count, head : 2 * head].astype(jnp.bfloat16)
        for j, b in enumerate(blocks):
            span = slice(j * rows, (j + 1) * rows)
            kv_own[place_of(b), 0] = keys[span]
            kv_own[place_of(b), 1] = values[span]

    def finish_queries(blocks):
        count = len(blocks) * rows
        queries = turned(count, 2, 0)
        cross = turned(count, 3, 2)
        for j, b in enumerate(blocks):
            span = slice(j * rows, (j + 1) * rows)
            q_all[b] = queries[span]
            c_all[b] = cross[span]

    def finish(blocks):
        finish_pairs(blocks)
        finish_queries(blocks)

    for i in range(CHUNKS):
        project(i, [me], i == 0)
    prepare_turn([me])
    finish([me])

    def gather_step(step, carry):
        before, after = block(-step), block(step)
        for slot in range(CHUNKS):
            for way in range(2):
                i = gather_chunk(way, slot)
                gather_arrival(way, step, i).wait_recv()
                if slot < CHUNKS // 2:
                    gather_copy(way, step, i).start()
                else:
                    pl.when(step < half - 1)(lambda way=way, i=i: gather_copy(way, step, i).start())
            if slot == 0:
                kv_copy(block(1 - step)).start()
                pl.when(step > 1)(lambda: kv_copy(block(step - 1)).start())
                prepare_turn([before, after])
            if slot >= CHUNKS // 2:
                project(gather_chunk(0, slot), [before, after], slot == CHUNKS // 2)
                project(gather_chunk(1, slot), [before, after], False)
        finish([before, after])
        return carry

    lax.fori_loop(1, half, gather_step, 0)
    kv_copy(block(1 - half)).start()
    kv_copy(block(half - 1)).start()
    last = block(half)
    prepare_turn([last])
    quiet = jnp.zeros((rows, cols), jnp.bfloat16)
    for i in range(CHUNKS):
        rs_in[(half if i < CHUNKS // 2 else 0) * CHUNKS + i] = quiet
    for slot in range(CHUNKS // 2):
        for way in range(2):
            i = gather_chunk(way, slot)
            gather_arrival(way, half, i).wait_recv()
            if slot < CHUNKS // 2 - 1:
                project(i, [last], slot == 0 and way == 0)
            else:
                project(i, [last], False, 0, 2)
    finish_pairs([last])
    kv_copy(last, 1).start()
    for way in range(2):
        project(gather_chunk(way, CHUNKS // 2 - 1), [last], False, 2, 4)
    finish_queries([last])

    def attend(queries, pairs, row):
        keys = pairs[:, 0].reshape(tokens, head)
        values = pairs[:, 1].reshape(tokens, head)
        scores = lax.dot_general(
            queries, keys, (((1,), (1,)), ((), ())), preferred_element_type=jnp.float32
        )
        scores = scores * score_scale + bias[row : row + 1, :]
        raised = jnp.exp2(scores - jnp.max(scores, -1, keepdims=True))
        total = jnp.sum(raised, -1, keepdims=True)
        summed = jnp.dot(raised.astype(jnp.bfloat16), values, preferred_element_type=jnp.float32)
        return (summed / total).astype(jnp.bfloat16)

    def scored(queries, keys, row, begin, end):
        scores = lax.dot_general(
            queries,
            keys.reshape(end - begin, head),
            (((1,), (1,)), ((), ())),
            preferred_element_type=jnp.float32,
        )
        return scores * score_scale + bias[row : row + 1, begin:end]

    def attend_self(blocks):
        picked = [q_all[b] for b in blocks]
        lhs = picked[0] if len(picked) == 1 else jnp.concatenate(picked, 0)
        both[: lhs.shape[0], :head] = attend(lhs, kv_own, 0)

    def attend_cross(blocks):
        picked = [c_all[b] for b in blocks]
        lhs = picked[0] if len(picked) == 1 else jnp.concatenate(picked, 0)
        both[: lhs.shape[0], head:] = attend(lhs, kv_far, 1)

    def expand(count, i):
        return jnp.dot(
            both[:count, :], w_out[:, i * cols : (i + 1) * cols], preferred_element_type=jnp.float32
        )

    def partial_piece(turn, blocks, piece):
        if piece == 0:
            attend_self(blocks)
        elif piece == 1:
            attend_cross(blocks)
        else:
            for i in range(2 * (piece - 2), 2 * (piece - 1)):
                term = expand(2 * rows, i)
                part[turn, 0, i] = term[:rows]
                part[turn, 1, i] = term[rows:]

    pltpu.make_async_copy(
        kv_far.at[pl.ds(0, n - 1)], kv_far.at[pl.ds(0, n - 1)], kv_recv.at[0]
    ).wait()
    split = n - max(128 // rows, 1)
    cross = c_all[last]
    early = scored(cross, kv_far[:split, 0], 1, 0, split * rows)
    attend_self([last])
    early_max = jnp.max(early, -1, keepdims=True)
    early = jnp.exp2(early - early_max)
    early_total = jnp.sum(early, -1, keepdims=True)
    early_sum = jnp.dot(
        early.astype(jnp.bfloat16),
        kv_far[:split, 1].reshape(split * rows, head),
        preferred_element_type=jnp.float32,
    )
    for i in range(CHUNKS):
        part[0, 0, i] = jnp.dot(
            both[:rows, :head],
            w_out[:head, i * cols : (i + 1) * cols],
            preferred_element_type=jnp.float32,
        )
    kv_copy(last, 1).wait_recv()
    late = scored(cross, kv_far[split:, 0], 1, split * rows, tokens)
    top = jnp.maximum(early_max, jnp.max(late, -1, keepdims=True))
    late = jnp.exp2(late - top)
    kept = jnp.exp2(early_max - top)
    total = kept * early_total + jnp.sum(late, -1, keepdims=True)
    summed = kept * early_sum + jnp.dot(
        late.astype(jnp.bfloat16),
        kv_far[split:, 1].reshape(tokens - split * rows, head),
        preferred_element_type=jnp.float32,
    )
    both[:rows, head:] = (summed / total).astype(jnp.bfloat16)
    for i in (0, 2, 1, 3):
        way = 0 if i < CHUNKS // 2 else 1
        term = part[0, 0, i] + jnp.dot(
            both[:rows, head:],
            w_out[head:, i * cols : (i + 1) * cols],
            preferred_element_type=jnp.float32,
        )
        rs_out[way * half * CHUNKS + i] = term.astype(jnp.bfloat16)
        scatter_copy(way, 0, i).start()
    for piece in range(4):
        partial_piece(1, [block(half - 1), block(1 - half)], piece)

    def scatter_step(step, carry):
        turn = lax.rem(step, 2)
        following = [block(half - 1 - step), block(step + 1 - half)]
        for slot in range(CHUNKS):
            for way in range(2):
                i = scatter_chunk(way, slot)
                if slot >= CHUNKS // 2:
                    scatter_copy(way, step - 1, i).wait_recv()
                else:
                    pl.when(step > 1)(lambda way=way, i=i: scatter_copy(way, step - 1, i).wait_recv())
                running = rs_in[(way * half + step - 1) * CHUNKS + i].astype(jnp.float32) + part[turn, way, i]
                rs_out[(way * half + step) * CHUNKS + i] = running.astype(jnp.bfloat16)
                scatter_copy(way, step, i).start()
            partial_piece(1 - turn, following, slot)
        return carry

    lax.fori_loop(1, half, scatter_step, 0)
    for i in (0, 2, 1, 3):
        scatter_copy(0, half - 1, i).wait_recv()
        scatter_copy(1, half - 1, i).wait_recv()
        span = slice(i * cols, (i + 1) * cols)
        branch = part[half % 2, 0, i] + (
            rs_in[(half - 1) * CHUNKS + i].astype(jnp.float32)
            + rs_in[(2 * half - 1) * CHUNKS + i].astype(jnp.float32)
        )
        out_ref[:, span] = (
            h_ref[:, span].astype(jnp.float32) + mod_ref[2, :, span] * branch
        ).astype(jnp.bfloat16)

    moved = (2 * half - 1) * CHUNKS
    all_sent(rows_all, moved, out_sem.at[0]).wait_send()
    all_sent(kv_own, n, out_sem.at[1]).wait_send()
    all_sent(rs_out, moved, out_sem.at[2]).wait_send()


def local(n, hidden, modulation, qk_gains, counts, offsets, in_weights, out_weights):
    rows, width = hidden.shape[1:]
    head = in_weights.shape[-1]
    half = n // 2
    tokens = n * rows
    cols = width // CHUNKS
    frequency = np.repeat(
        np.exp(np.arange(head // 2, dtype=np.float64) * (-2.0 * math.log(rope_base) / head)), 2
    ).astype(np.float32)[None]
    vmem = pl.BlockSpec(memory_space=pltpu.VMEM)
    anywhere = pl.BlockSpec(memory_space=pl.ANY)
    updated = pl.pallas_call(
        functools.partial(kernel, n),
        out_shape=pltpu.VMEM((rows, width), jnp.bfloat16),
        in_specs=[anywhere] * 8,
        out_specs=vmem,
        scratch_shapes=[
            pltpu.VMEM((rows, width), jnp.bfloat16),
            pltpu.VMEM((3, 1, width), jnp.float32),
            pltpu.VMEM((3, 1, head), jnp.float32),
            pltpu.VMEM((1, head), jnp.float32),
            pltpu.SMEM((1, 2), jnp.int32),
            pltpu.SMEM((1, 2), jnp.int32),
            pltpu.VMEM((n * CHUNKS, rows, cols), jnp.bfloat16),
            pltpu.VMEM((width * 4, head), jnp.bfloat16),
            pltpu.VMEM((4 * 128, head), jnp.float32),
            pltpu.VMEM((width, 4 * head), jnp.bfloat16),
            pltpu.VMEM((2 * head, width), jnp.bfloat16),
            pltpu.VMEM((2 * rows, 4 * head), jnp.float32),
            pltpu.VMEM((n, rows, head), jnp.bfloat16),
            pltpu.VMEM((n, rows, head), jnp.bfloat16),
            pltpu.VMEM((n, 2, rows, head), jnp.bfloat16),
            pltpu.VMEM((n, 2, rows, head), jnp.bfloat16),
            pltpu.VMEM((2, tokens), jnp.float32),
            pltpu.VMEM((2, 2 * rows, head), jnp.float32),
            pltpu.VMEM((2 * rows, 2 * head), jnp.bfloat16),
            pltpu.VMEM((2, 2, CHUNKS, rows, cols), jnp.float32),
            pltpu.VMEM((2 * half * CHUNKS, rows, cols), jnp.bfloat16),
            pltpu.VMEM((2 * half * CHUNKS, rows, cols), jnp.bfloat16),
            pltpu.SemaphoreType.DMA((8,)),
            pltpu.SemaphoreType.DMA((3,)),
            pltpu.SemaphoreType.DMA((2, 4, CHUNKS)),
            pltpu.SemaphoreType.DMA((2,)),
        ],
        compiler_params=pltpu.CompilerParams(
            collective_id=0, has_side_effects=True, vmem_limit_bytes=56 * 1024 * 1024
        ),
    )(
        hidden[0],
        jnp.transpose(modulation, (1, 0, 2)),
        jnp.transpose(qk_gains, (1, 0, 2)),
        jnp.asarray(frequency),
        counts.T,
        offsets.T,
        in_weights.reshape(4 * width, head),
        out_weights.reshape(2 * head, width),
    )
    return updated[None]


def solution(mesh):
    return jax.shard_map(
        functools.partial(local, mesh.shape["tp"]),
        mesh=mesh,
        in_specs=(
            P("tower", ("grp", "tp"), None),
            P("tower", None, None),
            P("tower", None, "tp"),
            P(None, "grp"),
            P(None, "grp"),
            P("tower", None, None, "tp"),
            P("tower", None, "tp", None),
        ),
        out_specs=P("tower", ("grp", "tp"), None),
        check_vma=False,
    )
```
